8 devices in a mesh: dp: 4 (over z, y, x), ep: 2 (over core).
Axes of the slice: x: 2, y: 2, z: 1, core: 2. Of those that a mesh axis runs over, the one named last changes fastest.
Arguments:
- x_norm: bfloat16 [2048, 1024], P(('dp', 'ep'))
- route_idx: int32 [2048, 8], P(('dp', 'ep'))
- w_router: bfloat16 [1024, 32], replicated
- w_gate: bfloat16 [32, 1024, 512], P('ep')
- w_up: bfloat16 [32, 1024, 512], P('ep')
- w_down: bfloat16 [32, 512, 1024], P('ep')
- grad_out: bfloat16 [2048, 1024], P(('dp', 'ep'))
Outputs:
- output 1: bfloat16 [2048, 1024], P(('dp', 'ep'))
- output 2: float32 [32, 1024, 512], P('ep')
- output 3: float32 [32, 1024, 512], P('ep')
- output 4: float32 [32, 512, 1024], P('ep')
- output 5: float32 [1024, 32], replicated
All inputs are finite; a program needn't handle non-finite values.
Results may differ from the reference program's by a relative error of at most 0.00616128.
Values are sent between devices in bfloat16 or wider.
A program may use at most 1 GiB of HBM per device.

```python
import jax
import jax.numpy as jnp
from jax import lax

D = 1024
FF = 512
EXPERTS = 32
TOP = 8
TOK_DEV = 256
SHARDS = 8
CAP = 192
TOKENS = SHARDS * TOK_DEV
N_CHOICE = TOKENS * TOP


def shuffle_rows(row_key):
    return jax.random.permutation(row_key, TOK_DEV)


def permute_rows(shard_rows, row_order):
    return shard_rows[row_order]


def draw_routes(route_key):
    perm_key, shift_key, order_key = jax.random.split(route_key, 3)
    expert_order = jax.random.permutation(perm_key, EXPERTS).astype(jnp.int32)
    shifts = jax.random.randint(shift_key, (SHARDS,), 0, EXPERTS - 1, dtype=jnp.int32)
    tok_pos = jnp.arange(TOK_DEV, dtype=jnp.int32)
    choice_pos = jnp.arange(TOP, dtype=jnp.int32)
    is_hot = tok_pos < CAP
    cycle_pos = (tok_pos * TOP - jnp.minimum(tok_pos, CAP))[:, None] + choice_pos[None, :] - is_hot[:, None].astype(jnp.int32)
    labels = 1 + (cycle_pos[None, :, :] + shifts[:, None, None]) % (EXPERTS - 1)
    hot_slot = is_hot[:, None] & (choice_pos[None, :] == 0)
    labels = jnp.where(hot_slot[None, :, :], 0, labels)
    experts = expert_order[labels]
    row_orders = jax.vmap(shuffle_rows)(jax.random.split(order_key, SHARDS))
    experts = jax.vmap(permute_rows)(experts, row_orders)
    return experts.reshape(TOKENS, TOP).astype(jnp.int32)


def setup_inputs(seed: int = 0) -> dict:
    base_key = jax.random.key(seed)
    key_list = jax.random.split(base_key, 7)
    x_norm = jax.random.normal(key_list[0], (TOKENS, D), jnp.float32)
    w_router = jax.random.normal(key_list[2], (D, EXPERTS), jnp.float32) * D ** -0.5
    w_gate = jax.random.normal(key_list[3], (EXPERTS, D, FF), jnp.float32) * D ** -0.5
    w_up = jax.random.normal(key_list[4], (EXPERTS, D, FF), jnp.float32) * D ** -0.5
    w_down = jax.random.normal(key_list[5], (EXPERTS, FF, D), jnp.float32) * FF ** -0.5
    grad_out = jax.random.normal(key_list[6], (TOKENS, D), jnp.float32)
    return {
        "x_norm": x_norm.astype(jnp.bfloat16),
        "route_idx": draw_routes(key_list[1]),
        "w_router": w_router.astype(jnp.bfloat16),
        "w_gate": w_gate.astype(jnp.bfloat16),
        "w_up": w_up.astype(jnp.bfloat16),
        "w_down": w_down.astype(jnp.bfloat16),
        "grad_out": grad_out.astype(jnp.bfloat16),
    }


def expert_backward(x_rows, dy_rows, gate_rows, w_gate_e, w_up_e, w_down_e):
    z_gate = jnp.dot(x_rows, w_gate_e, preferred_element_type=jnp.float32)
    z_up = jnp.dot(x_rows, w_up_e, preferred_element_type=jnp.float32)
    sigmoid_z = jax.nn.sigmoid(z_gate)
    silu_z = z_gate * sigmoid_z
    act_rows = (silu_z * z_up).astype(jnp.bfloat16)
    out_rows = jnp.dot(act_rows, w_down_e, preferred_element_type=jnp.float32)
    dy_wide = dy_rows.astype(jnp.float32)
    dgate_rows = jnp.sum(out_rows * dy_wide, axis=1)
    d_out = (gate_rows[:, None] * dy_wide).astype(jnp.bfloat16)
    d_act = jnp.dot(d_out, w_down_e.T, preferred_element_type=jnp.float32)
    d_zgate = (d_act * z_up * sigmoid_z * (1.0 + z_gate * (1.0 - sigmoid_z))).astype(jnp.bfloat16)
    d_zup = (d_act * silu_z).astype(jnp.bfloat16)
    dx_rows = (jnp.dot(d_zgate, w_gate_e.T, preferred_element_type=jnp.float32) + jnp.dot(d_zup, w_up_e.T, preferred_element_type=jnp.float32)).astype(jnp.bfloat16)
    grad_gate = jnp.dot(x_rows.T, d_zgate, preferred_element_type=jnp.float32)
    grad_up = jnp.dot(x_rows.T, d_zup, preferred_element_type=jnp.float32)
    grad_down = jnp.dot(act_rows.T, d_out, preferred_element_type=jnp.float32)
    return dx_rows, dgate_rows, grad_gate, grad_up, grad_down


def reference(x_norm, route_idx, w_router, w_gate, w_up, w_down, grad_out):
    logits = jnp.dot(x_norm, w_router, preferred_element_type=jnp.float32)
    gate_probs = jax.nn.softmax(jnp.take_along_axis(logits, route_idx, axis=1), axis=-1)
    expert_ids = jnp.arange(EXPERTS, dtype=jnp.int32)
    shard_idx = route_idx.reshape(SHARDS, TOK_DEV * TOP)
    one_hot = (shard_idx[:, :, None] == expert_ids).astype(jnp.int32)
    rank_in = jnp.sum((jnp.cumsum(one_hot, axis=1) - one_hot) * one_hot, axis=2)
    slot_ids = (shard_idx * (SHARDS * CAP) + jnp.arange(SHARDS, dtype=jnp.int32)[:, None] * CAP + rank_in).reshape(N_CHOICE)
    slot_table = jnp.full((EXPERTS * SHARDS * CAP,), N_CHOICE, jnp.int32).at[slot_ids].set(jnp.arange(N_CHOICE, dtype=jnp.int32)).reshape(EXPERTS, SHARDS * CAP)
    gate_flat = gate_probs.reshape(N_CHOICE)

    def one_expert(operands):
        w_gate_e, w_up_e, w_down_e, choice_ids = operands
        is_valid = choice_ids < N_CHOICE
        safe_ids = jnp.minimum(choice_ids, N_CHOICE - 1)
        x_rows = jnp.where(is_valid[:, None], x_norm[safe_ids // TOP], 0.0)
        dy_rows = jnp.where(is_valid[:, None], grad_out[safe_ids // TOP], 0.0)
        gate_rows = jnp.where(is_valid, gate_flat[safe_ids], 0.0)
        return expert_backward(x_rows, dy_rows, gate_rows, w_gate_e, w_up_e, w_down_e)

    dx_rows, dgate_rows, grad_gate, grad_up, grad_down = lax.map(one_expert, (w_gate, w_up, w_down, slot_table))
    dx_choice = dx_rows.reshape(EXPERTS * SHARDS * CAP, D)[slot_ids].reshape(TOKENS, TOP, D)
    dgate = dgate_rows.reshape(EXPERTS * SHARDS * CAP)[slot_ids].reshape(TOKENS, TOP)
    d_sel = gate_probs * (dgate - jnp.sum(gate_probs * dgate, axis=1, keepdims=True))
    d_logits = jnp.sum(jnp.where(route_idx[:, :, None] == expert_ids, d_sel[:, :, None], 0.0), axis=1).astype(jnp.bfloat16)
    du_router = jnp.dot(d_logits, w_router.T, preferred_element_type=jnp.float32)
    grad_x = (jnp.sum(dx_choice.astype(jnp.float32), axis=1) + du_router).astype(jnp.bfloat16)
    grad_router = jnp.dot(x_norm.T, d_logits, preferred_element_type=jnp.float32)
    return grad_x, grad_gate, grad_up, grad_down, grad_router
```

```python
import functools

import jax
import jax.numpy as jnp
from jax import lax
from jax.experimental import pallas as pl
from jax.experimental.pallas import tpu as pltpu
from jax.sharding import PartitionSpec as P

D = 1024
FF = 512
EXPERTS = 32
TOP = 8
TOK = 256
SHARDS = 8
E_LOC = 16
SLOT = 64
GROUP = 4
ROWS = SHARDS * SLOT
HOT = 128
CAP = 192
F32 = jnp.float32
BF16 = jnp.bfloat16


def dot_nn(a, b):
    return lax.dot_general(a, b, (((1,), (0,)), ((), ())), preferred_element_type=F32)


def dot_nt(a, b):
    return lax.dot_general(a, b, (((1,), (1,)), ((), ())), preferred_element_type=F32)


def dot_tn(a, b):
    return lax.dot_general(a, b, (((0,), (0,)), ((), ())), preferred_element_type=F32)


def route_tables(x_s, idx_t, w_router):
    logits = lax.dot_general(w_router, x_s, (((0,), (1,)), ((), ())), preferred_element_type=F32)
    e_iota = lax.broadcasted_iota(jnp.int32, (EXPERTS, TOK), 0)
    mask = e_iota == idx_t[0:1, :]
    for k in range(1, TOP):
        mask = mask | (e_iota == idx_t[k:k + 1, :])
    top = jnp.max(jnp.where(mask, logits, -jnp.inf), axis=0, keepdims=True)
    ex = jnp.where(mask, jnp.exp(jnp.where(mask, logits - top, 0.0)), 0.0)
    gates = ex / jnp.sum(ex, axis=0, keepdims=True)
    mask_f = jnp.where(mask, 1.0, 0.0)
    before = lax.broadcasted_iota(jnp.int32, (TOK, TOK), 0) < lax.broadcasted_iota(jnp.int32, (TOK, TOK), 1)
    rank = dot_nn(mask_f.astype(BF16), jnp.where(before, 1.0, 0.0).astype(BF16))
    code = jnp.where(mask, rank, -1.0)
    count = jnp.sum(mask_f, axis=1, keepdims=True)
    return code, gates, count


def main_kernel(info, x_ref, g_ref, idx_ref, wr_ref, w1_ref, w3_ref, w2_ref,
                o1_ref, o3_ref, o2_ref, s_ref, q_ref, gate_ref,
                code_s, gate_s, hot_s, list_s, xg_s, do_s, gg_s, r_s, a_s, dz1_s, dz3_s):
    i = pl.program_id(0)
    core = info[0]
    dp = info[1]
    e = core * E_LOC + i
    j = lax.rem(i, GROUP)

    def shard_of(b):
        return lax.rem(2 * dp + b, SHARDS)

    def slot_mask(b, ex, rows, base):
        row = code_s[b, pl.ds(ex, 1), :] - base
        r_iota = lax.broadcasted_iota(jnp.int32, (rows, TOK), 0).astype(F32)
        return row == r_iota

    def as_bf16(mask):
        return jnp.where(mask, 1.0, 0.0).astype(BF16)

    @pl.when(i == 0)
    def _():
        def prep(b, _):
            s = shard_of(b)
            code, gates, count = route_tables(x_ref[s], idx_ref[s], wr_ref[...])
            code_s[b] = code
            gate_s[b] = gates
            e_col = lax.broadcasted_iota(jnp.int32, (EXPERTS, 1), 0).astype(F32)
            hot_s[b] = jnp.max(jnp.where(count > SLOT, e_col, -1.0)).astype(jnp.int32)
            return 0
        lax.fori_loop(0, SHARDS, prep, 0)
        for b in range(2):
            gate_ref[b] = gate_s[b]
        s_ref[...] = jnp.zeros_like(s_ref)

    @pl.when(j == 0)
    def _():
        def gather(b, _):
            s = shard_of(b)
            masks = [slot_mask(b, e + jj, SLOT, 0.0) for jj in range(GROUP)]
            sel = jnp.concatenate([as_bf16(m) for m in masks], axis=0)
            xg = dot_nn(sel, x_ref[s]).astype(BF16)
            gg = dot_nn(sel, g_ref[s])
            row0 = pl.multiple_of(b * SLOT, SLOT)
            for jj in range(GROUP):
                part = slice(jj * SLOT, (jj + 1) * SLOT)
                xg_s[jj, pl.ds(row0, SLOT), :] = xg[part]
                p_col = jnp.sum(jnp.where(masks[jj], gate_s[b, pl.ds(e + jj, 1), :], 0.0), axis=1, keepdims=True)
                do_s[jj, pl.ds(row0, SLOT), :] = (p_col * gg[part]).astype(BF16)

            @pl.when(b < 2)
            def _():
                for jj in range(GROUP):
                    gg_s[jj, pl.ds(row0, SLOT), :] = gg[jj * SLOT:(jj + 1) * SLOT].astype(BF16)
            return 0
        lax.fori_loop(0, SHARDS, gather, 0)

    def compute(slot, first):
        x_rows = xg_s[slot]
        do_rows = do_s[slot]
        for n in range(2):
            cols = slice(n * 256, (n + 1) * 256)
            z1 = dot_nn(x_rows, w1_ref[0, :, cols])
            z3 = dot_nn(x_rows, w3_ref[0, :, cols])
            da = dot_nt(do_rows, w2_ref[0, cols, :])
            sig = jax.nn.sigmoid(z1)
            silu = z1 * sig
            a_s[:, cols] = (silu * z3).astype(BF16)
            dz1_s[:, cols] = (da * z3 * sig * (1.0 + z1 * (1.0 - sig))).astype(BF16)
            dz3_s[:, cols] = (da * silu).astype(BF16)
        g1 = dot_tn(x_rows, dz1_s[...])
        g3 = dot_tn(x_rows, dz3_s[...])
        g2 = dot_tn(a_s[...], do_rows)
        if first:
            o1_ref[0] = g1
            o3_ref[0] = g3
            o2_ref[0] = g2
        else:
            o1_ref[0] += g1
            o3_ref[0] += g3
            o2_ref[0] += g2

    def own_rows(row0, gg_rows):
        rows = pl.ds(row0, 2 * SLOT)
        o = dot_nn(a_s[rows, :], w2_ref[0])
        q = jnp.sum(o * gg_rows.astype(F32), axis=1, keepdims=True)
        dx = (dot_nt(dz1_s[rows, :], w1_ref[0]) + dot_nt(dz3_s[rows, :], w3_ref[0])).astype(BF16)
        return q, dx

    compute(j, True)
    q, dx = own_rows(0, gg_s[j])
    for b in range(2):
        part = slice(b * SLOT, (b + 1) * SLOT)
        r_s[b, pl.ds(pl.multiple_of(j * SLOT, SLOT), SLOT), :] = dx[part]
        q_ref[b, pl.ds(i, 1), :] = jnp.sum(jnp.where(slot_mask(b, e, SLOT, 0.0), q[part], 0.0), axis=0, keepdims=True)

    @pl.when(j == GROUP - 1)
    def _():
        for b in range(2):
            sel = jnp.concatenate([as_bf16(slot_mask(b, e - (GROUP - 1) + jj, SLOT, 0.0)) for jj in range(GROUP)], axis=0)
            s_ref[b] += dot_tn(sel, r_s[b])

    n_hot = jnp.int32(0)
    for b in range(SHARDS):
        list_s[b] = jnp.int32(0)
    for b in range(SHARDS):
        hit = hot_s[b] == e

        @pl.when(hit)
        def _(b=b, n_hot=n_hot):
            list_s[n_hot] = jnp.int32(b)
        n_hot = n_hot + hit.astype(jnp.int32)

    def hot_chunk(c, _):
        def gather(k, _):
            pos = c * 4 + k
            b = list_s[pos]
            s = shard_of(b)
            live = pos < n_hot
            mask = slot_mask(b, e, HOT, jnp.where(live, float(SLOT), 4096.0))
            sel = as_bf16(mask)
            rows = pl.ds(pl.multiple_of(k * HOT, HOT), HOT)
            xg_s[GROUP, rows, :] = dot_nn(sel, x_ref[s]).astype(BF16)
            gg = dot_nn(sel, g_ref[s])
            p_col = jnp.sum(jnp.where(mask, gate_s[b, pl.ds(e, 1), :], 0.0), axis=1, keepdims=True)
            do_s[GROUP, rows, :] = (p_col * gg).astype(BF16)

            @pl.when(k < 2)
            def _():
                gg_s[GROUP + k] = gg.astype(BF16)
            return 0
        lax.fori_loop(0, 4, gather, 0)
        compute(GROUP, False)

        def own(k, _):
            b = list_s[k]

            @pl.when((c == 0) & (k < n_hot) & (b < 2))
            def _():
                q, dx = own_rows(pl.multiple_of(k * HOT, HOT), gg_s[GROUP + k])
                mask = slot_mask(b, e, HOT, float(SLOT))
                s_ref[b] += dot_tn(as_bf16(mask), dx)
                q_ref[b, pl.ds(i, 1), :] += jnp.sum(jnp.where(mask, q, 0.0), axis=0, keepdims=True)
            return 0
        lax.fori_loop(0, 2, own, 0)
        return 0

    lax.fori_loop(0, lax.div(n_hot + 3, 4), hot_chunk, 0)


def expert_pass(info, x_all, g_all, idx_all, w_router, w_gate, w_up, w_down):
    vmem = pl.BlockSpec(memory_space=pltpu.VMEM)
    up_spec = pl.BlockSpec((1, D, FF), lambda i, info: (i, 0, 0))
    down_spec = pl.BlockSpec((1, FF, D), lambda i, info: (i, 0, 0))
    return pl.pallas_call(
        main_kernel,
        out_shape=(
            jax.ShapeDtypeStruct((E_LOC, D, FF), F32),
            jax.ShapeDtypeStruct((E_LOC, D, FF), F32),
            jax.ShapeDtypeStruct((E_LOC, FF, D), F32),
            jax.ShapeDtypeStruct((2, TOK, D), F32),
            jax.ShapeDtypeStruct((2, E_LOC, TOK), F32),
            jax.ShapeDtypeStruct((2, EXPERTS, TOK), F32),
        ),
        grid_spec=pltpu.PrefetchScalarGridSpec(
            num_scalar_prefetch=1,
            grid=(E_LOC,),
            in_specs=[vmem, vmem, vmem, vmem, up_spec, up_spec, down_spec],
            out_specs=(up_spec, up_spec, down_spec, vmem, vmem, vmem),
            scratch_shapes=[
                pltpu.VMEM((SHARDS, EXPERTS, TOK), F32),
                pltpu.VMEM((SHARDS, EXPERTS, TOK), F32),
                pltpu.SMEM((SHARDS,), jnp.int32),
                pltpu.SMEM((SHARDS,), jnp.int32),
                pltpu.VMEM((GROUP + 1, ROWS, D), BF16),
                pltpu.VMEM((GROUP + 1, ROWS, D), BF16),
                pltpu.VMEM((GROUP + 2, 2 * SLOT, D), BF16),
                pltpu.VMEM((2, GROUP * SLOT, D), BF16),
                pltpu.VMEM((ROWS, FF), BF16),
                pltpu.VMEM((ROWS, FF), BF16),
                pltpu.VMEM((ROWS, FF), BF16),
            ],
        ),
        compiler_params=pltpu.CompilerParams(
            dimension_semantics=("arbitrary",), vmem_limit_bytes=64_000_000),
        cost_estimate=pl.CostEstimate(flops=90_000_000_000, bytes_accessed=170_000_000, transcendentals=8_000_000),
        name="experts",
    )(info, x_all, g_all, idx_all, w_router, w_gate, w_up, w_down)


def solution(mesh):
    tok_spec = P(("dp", "ep"), None)
    exp_spec = P("ep", None, None)

    def device_step(x_loc, route_idx, w_router, w_gate, w_up, w_down, dy_loc):
        core = lax.axis_index("ep")
        dp = lax.axis_index("dp")
        info = jnp.stack([core, dp]).astype(jnp.int32)
        x_all = lax.all_gather(x_loc, ("dp", "ep"))
        g_all = lax.all_gather(dy_loc, ("dp", "ep"))
        idx_all = lax.all_gather(route_idx.T, ("dp", "ep"))
        g1, g3, g2, dx_part, q_part, gates = expert_pass(info, x_all, g_all, idx_all, w_router, w_gate, w_up, w_down)
        swap = [(0, 1), (1, 0)]
        mine = lambda v: lax.dynamic_index_in_dim(v, core, 0, keepdims=False)
        other = lambda v: lax.ppermute(lax.dynamic_index_in_dim(v, 1 - core, 0, keepdims=False), "ep", swap)
        q_mine, q_other = mine(q_part), other(q_part)
        q_all = jnp.where(core == 0, jnp.concatenate([q_mine, q_other]), jnp.concatenate([q_other, q_mine]))
        p_all = mine(gates)
        d_log = (p_all * (q_all - jnp.sum(p_all * q_all, axis=0, keepdims=True))).astype(BF16)
        du = lax.dot_general(d_log, w_router, (((0,), (1,)), ((), ())), preferred_element_type=F32)
        grad_x = (mine(dx_part) + other(dx_part) + du).astype(BF16)
        d_log_all = lax.all_gather(d_log, ("dp", "ep"))
        grad_router = lax.dot_general(x_all, d_log_all, (((0, 1), (0, 2)), ((), ())), preferred_element_type=F32)
        return grad_x, g1, g3, g2, grad_router

    return jax.shard_map(device_step, mesh=mesh, in_specs=(tok_spec, tok_spec, P(), exp_spec, exp_spec, exp_spec, tok_spec), out_specs=(tok_spec, exp_spec, exp_spec, exp_spec, P()), check_vma=False)
```

```python
import jax
import jax.numpy as jnp
from jax import lax
from jax.experimental import pallas as pl
from jax.experimental.pallas import tpu as pltpu
from jax.sharding import PartitionSpec as P

D = 1024
FF = 512
EXPERTS = 32
TOP = 8
TOK = 256
SHARDS = 8
E_LOC = 16
SLOT = 64
GROUP = 4
ROWS = SHARDS * SLOT
HOT = 128
CAP = 192
F32 = jnp.float32
BF16 = jnp.bfloat16
MESH = pl.DeviceIdType.MESH


def dot_nn(a, b):
    return lax.dot_general(a, b, (((1,), (0,)), ((), ())), preferred_element_type=F32)


def dot_nt(a, b):
    return lax.dot_general(a, b, (((1,), (1,)), ((), ())), preferred_element_type=F32)


def dot_tn(a, b):
    return lax.dot_general(a, b, (((0,), (0,)), ((), ())), preferred_element_type=F32)


def route_tables(x_s, idx_t, w_router):
    logits = lax.dot_general(w_router, x_s, (((0,), (1,)), ((), ())), preferred_element_type=F32)
    e_iota = lax.broadcasted_iota(jnp.int32, (EXPERTS, TOK), 0)
    mask = e_iota == idx_t[0:1, :]
    for k in range(1, TOP):
        mask = mask | (e_iota == idx_t[k:k + 1, :])
    top = jnp.max(jnp.where(mask, logits, -jnp.inf), axis=0, keepdims=True)
    ex = jnp.where(mask, jnp.exp(jnp.where(mask, logits - top, 0.0)), 0.0)
    gates = ex / jnp.sum(ex, axis=0, keepdims=True)
    mask_f = jnp.where(mask, 1.0, 0.0)
    before = lax.broadcasted_iota(jnp.int32, (TOK, TOK), 0) < lax.broadcasted_iota(jnp.int32, (TOK, TOK), 1)
    rank = dot_nn(mask_f.astype(BF16), jnp.where(before, 1.0, 0.0).astype(BF16))
    code = jnp.where(mask, rank, -1.0)
    count = jnp.sum(mask_f, axis=1, keepdims=True)
    return code, gates, count


def main_kernel(info, x_ref, g_ref, idx_ref, wr_ref, w1_ref, w3_ref, w2_ref,
                o1_ref, o3_ref, o2_ref, s_ref, q_ref, gate_ref,
                code_s, gate_s, hot_s, list_s, xg_s, do_s, gg_s, r_s, a_s, dz1_s, dz3_s):
    i = pl.program_id(0)
    e = info[0] * E_LOC + i
    j = lax.rem(i, GROUP)

    def slot_mask(b, ex, rows, base):
        row = code_s[b, pl.ds(ex, 1), :] - base
        r_iota = lax.broadcasted_iota(jnp.int32, (rows, TOK), 0).astype(F32)
        return row == r_iota

    def as_bf16(mask):
        return jnp.where(mask, 1.0, 0.0).astype(BF16)

    @pl.when(i == 0)
    def _():
        def prep(b, _):
            code, gates, count = route_tables(x_ref[b], idx_ref[b], wr_ref[...])
            code_s[b] = code
            gate_s[b] = gates
            e_col = lax.broadcasted_iota(jnp.int32, (EXPERTS, 1), 0).astype(F32)
            hot_s[b] = jnp.max(jnp.where(count > SLOT, e_col, -1.0)).astype(jnp.int32)
            return 0
        lax.fori_loop(0, SHARDS, prep, 0)
        for b in range(2):
            gate_ref[b] = gate_s[b]
        s_ref[...] = jnp.zeros_like(s_ref)

    @pl.when(j == 0)
    def _():
        def gather(b, _):
            masks = [slot_mask(b, e + jj, SLOT, 0.0) for jj in range(GROUP)]
            sel = jnp.concatenate([as_bf16(m) for m in masks], axis=0)
            xg = dot_nn(sel, x_ref[b]).astype(BF16)
            gg = dot_nn(sel, g_ref[b])
            row0 = pl.multiple_of(b * SLOT, SLOT)
            for jj in range(GROUP):
                part = slice(jj * SLOT, (jj + 1) * SLOT)
                xg_s[jj, pl.ds(row0, SLOT), :] = xg[part]
                p_col = jnp.sum(jnp.where(masks[jj], gate_s[b, pl.ds(e + jj, 1), :], 0.0), axis=1, keepdims=True)
                do_s[jj, pl.ds(row0, SLOT), :] = (p_col * gg[part]).astype(BF16)

            @pl.when(b < 2)
            def _():
                for jj in range(GROUP):
                    gg_s[jj, pl.ds(row0, SLOT), :] = gg[jj * SLOT:(jj + 1) * SLOT].astype(BF16)
            return 0
        lax.fori_loop(0, SHARDS, gather, 0)

    def compute(slot, first):
        x_rows = xg_s[slot]
        do_rows = do_s[slot]
        for n in range(2):
            cols = slice(n * 256, (n + 1) * 256)
            z1 = dot_nn(x_rows, w1_ref[0, :, cols])
            z3 = dot_nn(x_rows, w3_ref[0, :, cols])
            da = dot_nt(do_rows, w2_ref[0, cols, :])
            sig = jax.nn.sigmoid(z1)
            silu = z1 * sig
            a_s[:, cols] = (silu * z3).astype(BF16)
            dz1_s[:, cols] = (da * z3 * sig * (1.0 + z1 * (1.0 - sig))).astype(BF16)
            dz3_s[:, cols] = (da * silu).astype(BF16)
        g1 = dot_tn(x_rows, dz1_s[...])
        g3 = dot_tn(x_rows, dz3_s[...])
        g2 = dot_tn(a_s[...], do_rows)
        if first:
            o1_ref[0] = g1
            o3_ref[0] = g3
            o2_ref[0] = g2
        else:
            o1_ref[0] += g1
            o3_ref[0] += g3
            o2_ref[0] += g2

    def own_rows(row0, gg_rows):
        rows = pl.ds(row0, 2 * SLOT)
        o = dot_nn(a_s[rows, :], w2_ref[0])
        q = jnp.sum(o * gg_rows.astype(F32), axis=1, keepdims=True)
        dx = (dot_nt(dz1_s[rows, :], w1_ref[0]) + dot_nt(dz3_s[rows, :], w3_ref[0])).astype(BF16)
        return q, dx

    compute(j, True)
    q, dx = own_rows(0, gg_s[j])
    for b in range(2):
        part = slice(b * SLOT, (b + 1) * SLOT)
        r_s[b, pl.ds(pl.multiple_of(j * SLOT, SLOT), SLOT), :] = dx[part]
        q_ref[b, pl.ds(i, 1), :] = jnp.sum(jnp.where(slot_mask(b, e, SLOT, 0.0), q[part], 0.0), axis=0, keepdims=True)

    @pl.when(j == GROUP - 1)
    def _():
        for b in range(2):
            sel = jnp.concatenate([as_bf16(slot_mask(b, e - (GROUP - 1) + jj, SLOT, 0.0)) for jj in range(GROUP)], axis=0)
            s_ref[b] += dot_tn(sel, r_s[b])

    n_hot = jnp.int32(0)
    for b in range(SHARDS):
        list_s[b] = jnp.int32(0)
    for b in range(SHARDS):
        hit = hot_s[b] == e

        @pl.when(hit)
        def _(b=b, n_hot=n_hot):
            list_s[n_hot] = jnp.int32(b)
        n_hot = n_hot + hit.astype(jnp.int32)

    def hot_chunk(c, _):
        def gather(k, _):
            pos = c * 4 + k
            b = list_s[pos]
            live = pos < n_hot
            mask = slot_mask(b, e, HOT, jnp.where(live, float(SLOT), 4096.0))
            sel = as_bf16(mask)
            rows = pl.ds(pl.multiple_of(k * HOT, HOT), HOT)
            xg_s[GROUP, rows, :] = dot_nn(sel, x_ref[b]).astype(BF16)
            gg = dot_nn(sel, g_ref[b])
            p_col = jnp.sum(jnp.where(mask, gate_s[b, pl.ds(e, 1), :], 0.0), axis=1, keepdims=True)
            do_s[GROUP, rows, :] = (p_col * gg).astype(BF16)

            @pl.when(k < 2)
            def _():
                gg_s[GROUP + k] = gg.astype(BF16)
            return 0
        lax.fori_loop(0, 4, gather, 0)
        compute(GROUP, False)

        def own(k, _):
            b = list_s[k]

            @pl.when((c == 0) & (k < n_hot) & (b < 2))
            def _():
                q, dx = own_rows(pl.multiple_of(k * HOT, HOT), gg_s[GROUP + k])
                mask = slot_mask(b, e, HOT, float(SLOT))
                s_ref[b] += dot_tn(as_bf16(mask), dx)
                q_ref[b, pl.ds(i, 1), :] += jnp.sum(jnp.where(mask, q, 0.0), axis=0, keepdims=True)
            return 0
        lax.fori_loop(0, 2, own, 0)
        return 0

    lax.fori_loop(0, lax.div(n_hot + 3, 4), hot_chunk, 0)


def expert_pass(info, x_all, g_all, idx_all, w_router, w_gate, w_up, w_down):
    vmem = pl.BlockSpec(memory_space=pltpu.VMEM)
    up_spec = pl.BlockSpec((1, D, FF), lambda i, info: (i, 0, 0))
    down_spec = pl.BlockSpec((1, FF, D), lambda i, info: (i, 0, 0))
    return pl.pallas_call(
        main_kernel,
        out_shape=(
            jax.ShapeDtypeStruct((E_LOC, D, FF), F32),
            jax.ShapeDtypeStruct((E_LOC, D, FF), F32),
            jax.ShapeDtypeStruct((E_LOC, FF, D), F32),
            jax.ShapeDtypeStruct((2, TOK, D), F32),
            jax.ShapeDtypeStruct((2, E_LOC, TOK), F32),
            jax.ShapeDtypeStruct((2, EXPERTS, TOK), F32),
        ),
        grid_spec=pltpu.PrefetchScalarGridSpec(
            num_scalar_prefetch=1,
            grid=(E_LOC,),
            in_specs=[vmem, vmem, vmem, vmem, up_spec, up_spec, down_spec],
            out_specs=(up_spec, up_spec, down_spec, vmem, vmem, vmem),
            scratch_shapes=[
                pltpu.VMEM((SHARDS, EXPERTS, TOK), F32),
                pltpu.VMEM((SHARDS, EXPERTS, TOK), F32),
                pltpu.SMEM((SHARDS,), jnp.int32),
                pltpu.SMEM((SHARDS,), jnp.int32),
                pltpu.VMEM((GROUP + 1, ROWS, D), BF16),
                pltpu.VMEM((GROUP + 1, ROWS, D), BF16),
                pltpu.VMEM((GROUP + 2, 2 * SLOT, D), BF16),
                pltpu.VMEM((2, GROUP * SLOT, D), BF16),
                pltpu.VMEM((ROWS, FF), BF16),
                pltpu.VMEM((ROWS, FF), BF16),
                pltpu.VMEM((ROWS, FF), BF16),
            ],
        ),
        compiler_params=pltpu.CompilerParams(
            dimension_semantics=("arbitrary",), vmem_limit_bytes=64_000_000),
        cost_estimate=pl.CostEstimate(flops=90_000_000_000, bytes_accessed=170_000_000, transcendentals=8_000_000),
        name="experts",
    )(info, x_all, g_all, idx_all, w_router, w_gate, w_up, w_down)


def peer(step):
    chip = lax.axis_index("dp")
    core = lax.axis_index("ep")
    x_bit, y_bit = lax.rem(chip, 2), lax.div(chip, 2)
    if step & 2:
        x_bit = 1 - x_bit
    if step & 4:
        y_bit = 1 - y_bit
    if step & 1:
        core = 1 - core
    return {"dp": 2 * y_bit + x_bit, "ep": core}


def greet_all():
    barrier = pltpu.get_barrier_semaphore()
    for step in range(1, SHARDS):
        pl.semaphore_signal(barrier, inc=1, device_id=peer(step), device_id_type=MESH)
    pl.semaphore_wait(barrier, SHARDS - 1)


def share_kernel(x_ref, g_ref, idx_ref, x_all, g_all, idx_all, send, recv, local):
    def copy(ref, into, sem, slot, step):
        return pltpu.make_async_remote_copy(
            src_ref=ref, dst_ref=into.at[slot], send_sem=send.at[sem], recv_sem=recv.at[sem],
            device_id=peer(step), device_id_type=MESH)

    own = [pltpu.make_async_copy(ref, into.at[0], local.at[n])
           for n, (ref, into) in enumerate(((x_ref, x_all), (g_ref, g_all), (idx_ref, idx_all)))]
    for c in own:
        c.start()
    greet_all()
    ids = [copy(idx_ref, idx_all, 14 + k - 1, k, k) for k in range(1, SHARDS)]
    for c in ids:
        c.start()
    x1, g1 = copy(x_ref, x_all, 0, 1, 1), copy(g_ref, g_all, 7, 1, 1)
    x2, g2 = copy(x_ref, x_all, 1, 2, 2), copy(g_ref, g_all, 8, 2, 2)
    g4, x4 = copy(g_ref, g_all, 10, 4, 4), copy(x_ref, x_all, 3, 4, 4)
    x6, g6 = copy(x_all.at[2], x_all, 5, 6, 4), copy(g_all.at[4], g_all, 12, 6, 2)
    x3, g3 = copy(x_all.at[2], x_all, 2, 3, 1), copy(g_all.at[2], g_all, 9, 3, 1)
    x5, g5 = copy(x_all.at[4], x_all, 4, 5, 1), copy(g_all.at[4], g_all, 11, 5, 1)
    x7, g7 = copy(x_all.at[6], x_all, 6, 7, 1), copy(g_all.at[6], g_all, 13, 7, 1)
    for c in (x1, g1, x2, g4, g2, x4):
        c.start()
    x2.wait_recv()
    x6.start()
    x3.start()
    g4.wait_recv()
    g6.start()
    g5.start()
    g2.wait_recv()
    g3.start()
    x4.wait_recv()
    x5.start()
    x6.wait_recv()
    x7.start()
    g6.wait_recv()
    g7.start()
    for c in (x1, g1, x3, g3, x5, g5, x7, g7, *ids):
        c.wait_recv()
    for c in (x1, g1, x2, g2, g4, x4, x6, g6, x3, g3, x5, g5, x7, g7, *ids):
        c.wait_send()
    for c in own:
        c.wait()


def share_tokens(x_loc, dy_loc, idx_t):
    vmem = pl.BlockSpec(memory_space=pltpu.VMEM)
    hbm = pl.BlockSpec(memory_space=pl.ANY)
    return pl.pallas_call(
        share_kernel,
        out_shape=(
            jax.ShapeDtypeStruct((SHARDS, TOK, D), BF16),
            jax.ShapeDtypeStruct((SHARDS, TOK, D), BF16),
            jax.ShapeDtypeStruct((SHARDS, TOP, TOK), jnp.int32),
        ),
        in_specs=[vmem, vmem, vmem],
        out_specs=(hbm, hbm, hbm),
        scratch_shapes=[
            pltpu.SemaphoreType.DMA((21,)),
            pltpu.SemaphoreType.DMA((21,)),
            pltpu.SemaphoreType.DMA((3,)),
        ],
        compiler_params=pltpu.CompilerParams(collective_id=0, has_side_effects=True),
        name="share",
    )(x_loc, dy_loc, idx_t)


def tail_kernel(s_ref, q_ref, gate_ref, x_all, wr_ref, gx_ref, gr_ref, s_got, q_got, dl_all, send, recv):
    core = lax.axis_index("ep")

    def copy(ref, into, sem, step):
        return pltpu.make_async_remote_copy(
            src_ref=ref, dst_ref=into, send_sem=send.at[sem], recv_sem=recv.at[sem],
            device_id=peer(step), device_id_type=MESH)

    greet_all()
    q_copy = copy(q_ref.at[1], q_got, 0, 1)
    s_copy = copy(s_ref.at[1], s_got, 1, 1)
    q_copy.start()
    s_copy.start()
    q_copy.wait_recv()
    low = jnp.concatenate([q_ref[0], q_got[...]], axis=0)
    high = jnp.concatenate([q_got[...], q_ref[0]], axis=0)
    q = jnp.where(core == 0, low, high)
    p = gate_ref[0]
    d_log = (p * (q - jnp.sum(p * q, axis=0, keepdims=True))).astype(BF16)
    dl_all[0] = d_log
    copies = [copy(dl_all.at[0], dl_all.at[k], 1 + k, k) for k in range(1, SHARDS)]
    for c in copies:
        c.start()
    du = lax.dot_general(d_log, wr_ref[...], (((0,), (1,)), ((), ())), preferred_element_type=F32)
    s_copy.wait_recv()
    gx_ref[...] = (s_ref[0] + s_got[...] + du).astype(BF16)
    total = lax.dot_general(x_all[0], d_log, (((0,), (1,)), ((), ())), preferred_element_type=F32)
    for k in range(1, SHARDS):
        copies[k - 1].wait_recv()
        total += lax.dot_general(x_all[k], dl_all[k], (((0,), (1,)), ((), ())), preferred_element_type=F32)
    gr_ref[...] = total
    q_copy.wait_send()
    s_copy.wait_send()
    for c in copies:
        c.wait_send()


def tail(dx_part, q_part, gates, x_all, w_router):
    vmem = pl.BlockSpec(memory_space=pltpu.VMEM)
    return pl.pallas_call(
        tail_kernel,
        out_shape=(jax.ShapeDtypeStruct((TOK, D), BF16), jax.ShapeDtypeStruct((D, EXPERTS), F32)),
        in_specs=[vmem] * 5,
        out_specs=(vmem, vmem),
        scratch_shapes=[
            pltpu.VMEM((TOK, D), F32),
            pltpu.VMEM((E_LOC, TOK), F32),
            pltpu.VMEM((SHARDS, EXPERTS, TOK), BF16),
            pltpu.SemaphoreType.DMA((9,)),
            pltpu.SemaphoreType.DMA((9,)),
        ],
        compiler_params=pltpu.CompilerParams(collective_id=1, has_side_effects=True, vmem_limit_bytes=32_000_000),
        name="tail",
    )(dx_part, q_part, gates, x_all, w_router)


def solution(mesh):
    tok_spec = P(("dp", "ep"), None)
    exp_spec = P("ep", None, None)

    def device_step(x_loc, route_idx, w_router, w_gate, w_up, w_down, dy_loc):
        info = lax.axis_index("ep").astype(jnp.int32).reshape(1)
        x_all, g_all, idx_all = share_tokens(x_loc, dy_loc, route_idx.T)
        g1, g3, g2, dx_part, q_part, gates = expert_pass(info, x_all, g_all, idx_all, w_router, w_gate, w_up, w_down)
        grad_x, grad_router = tail(dx_part, q_part, gates, x_all, w_router)
        return grad_x, g1, g3, g2, grad_router

    return jax.shard_map(device_step, mesh=mesh, in_specs=(tok_spec, tok_spec, P(), exp_spec, exp_spec, exp_spec, tok_spec), out_specs=(tok_spec, exp_spec, exp_spec, exp_spec, P()), check_vma=False)
```

```python
import jax
import jax.numpy as jnp
from jax import lax
from jax.experimental import pallas as pl
from jax.experimental.pallas import tpu as pltpu
from jax.sharding import PartitionSpec as P

D = 1024
FF = 512
EXPERTS = 32
TOP = 8
TOK = 256
SHARDS = 8
E_LOC = 16
SLOT = 64
GROUP = 4
ROWS = SHARDS * SLOT
HOT = 128
OWN = 2 * SLOT
FORWARD = (5, 9, 14)
VMEM_ALL = 67_000_000
CAP = 192
F32 = jnp.float32
BF16 = jnp.bfloat16
MESH = pl.DeviceIdType.MESH


def dot_nn(a, b):
    return lax.dot_general(a, b, (((1,), (0,)), ((), ())), preferred_element_type=F32)


def dot_nt(a, b):
    return lax.dot_general(a, b, (((1,), (1,)), ((), ())), preferred_element_type=F32)


def dot_tn(a, b):
    return lax.dot_general(a, b, (((0,), (0,)), ((), ())), preferred_element_type=F32)


def route_tables(x_s, idx_t, w_router_t):
    logits = dot_nt(w_router_t, x_s)
    e_iota = lax.broadcasted_iota(jnp.int32, (EXPERTS, TOK), 0)
    mask = e_iota == idx_t[0:1, :]
    for k in range(1, TOP):
        mask = mask | (e_iota == idx_t[k:k + 1, :])
    top = jnp.max(jnp.where(mask, logits, -jnp.inf), axis=0, keepdims=True)
    ex = jnp.where(mask, jnp.exp(jnp.where(mask, logits - top, 0.0)), 0.0)
    gates = ex / jnp.sum(ex, axis=0, keepdims=True)
    mask_f = jnp.where(mask, 1.0, 0.0)
    before = lax.broadcasted_iota(jnp.int32, (TOK, TOK), 0) < lax.broadcasted_iota(jnp.int32, (TOK, TOK), 1)
    rank = dot_nn(mask_f.astype(BF16), jnp.where(before, 1.0, 0.0).astype(BF16))
    code = jnp.where(mask, rank, -1.0)
    count = jnp.sum(mask_f, axis=1, keepdims=True)
    return code, gates, count


def slot_mask(code_row, rows, base):
    r_iota = lax.broadcasted_iota(jnp.int32, (rows, TOK), 0).astype(F32)
    return code_row - base == r_iota


def as_bf16(mask):
    return jnp.where(mask, 1.0, 0.0).astype(BF16)


def swiglu_grads(z1, z3, da):
    sig = jax.nn.sigmoid(z1)
    silu = z1 * sig
    act = (silu * z3).astype(BF16)
    dz1 = (da * z3 * sig * (1.0 + z1 * (1.0 - sig))).astype(BF16)
    dz3 = (da * silu).astype(BF16)
    return act, dz1, dz3


def own_grads(act, dz1, dz3, gg, w1, w3, w2):
    o = dot_nn(act, w2)
    q = jnp.sum(o * gg.astype(F32), axis=1, keepdims=True)
    dx = (dot_nt(dz1, w1) + dot_nt(dz3, w3)).astype(BF16)
    return q, dx


def main_kernel(info, x_hbm, g_hbm, idx_ref, wr_ref, s_hbm, q_in, own_x, own_do, own_a, own_dz1, own_dz3,
                w1_ref, w3_ref, w2_ref, o1_ref, o3_ref, o2_ref, s_ref, q_ref,
                x_s, g_s, code_s, gate_s, hot_s, list_s, xg_s, do_s, xh_s, dh_s, gg_s, a_s, dz1_s, dz3_s, sem):
    i = pl.program_id(0)
    e = info[0] * E_LOC + i
    j = lax.rem(i, GROUP)
    buf = lax.rem(lax.div(i, GROUP), 2)

    def load(ref, into, b, n):
        return pltpu.make_async_copy(ref.at[b], into.at[b], sem.at[n, b])

    s_load = pltpu.make_async_copy(s_hbm, s_ref, sem.at[2, 0])

    def select(b, ex, rows, base):
        return slot_mask(code_s[b, pl.ds(ex, 1), :], rows, base)

    def gather(b, first, into):
        masks = [select(b, first + jj, SLOT, 0.0) for jj in range(GROUP)]
        sel = jnp.concatenate([as_bf16(m) for m in masks], axis=0)
        xg = dot_nn(sel, x_s[b]).astype(BF16)
        gg = dot_nn(sel, g_s[b])
        row0 = pl.multiple_of(b * SLOT, SLOT)
        for jj in range(GROUP):
            part = slice(jj * SLOT, (jj + 1) * SLOT)
            xg_s[into, jj, pl.ds(row0, SLOT), :] = xg[part]
            p_col = jnp.sum(jnp.where(masks[jj], gate_s[b, pl.ds(first + jj, 1), :], 0.0), axis=1, keepdims=True)
            do_s[into, jj, pl.ds(row0, SLOT), :] = (p_col * gg[part]).astype(BF16)

    @pl.when(i == 0)
    def _():
        for b in range(SHARDS):
            load(x_hbm, x_s, b, 0).start()
            load(g_hbm, g_s, b, 1).start()
        s_load.start()

        def prep(b, _):
            load(x_hbm, x_s, b, 0).wait()
            code, gates, count = route_tables(x_s[b], idx_ref[b], wr_ref[...])
            code_s[b] = code
            gate_s[b] = gates
            e_col = lax.broadcasted_iota(jnp.int32, (EXPERTS, 1), 0).astype(F32)
            hot_s[b] = jnp.max(jnp.where(count > SLOT, e_col, -1.0)).astype(jnp.int32)
            load(g_hbm, g_s, b, 1).wait()
            return 0
        lax.fori_loop(0, SHARDS, prep, 0)
        q_ref[...] = q_in[...]

        def first_gather(b, _):
            gather(b, e, 0)
            return 0
        lax.fori_loop(2, SHARDS, first_gather, 0)
        s_load.wait()

    @pl.when((i < E_LOC - GROUP) & (j < 3))
    def _():
        for k in range(2):
            gather(2 + 2 * j + k, e - j + GROUP, 1 - buf)

    def compute(x_at, do_at, first):
        skip = OWN if first else 0
        rest = slice(skip, ROWS)
        for n in range(2):
            cols = slice(n * 256, (n + 1) * 256)
            z1 = dot_nn(x_at[rest, :], w1_ref[0, :, cols])
            z3 = dot_nn(x_at[rest, :], w3_ref[0, :, cols])
            da = dot_nt(do_at[rest, :], w2_ref[0, cols, :])
            act, dz1, dz3 = swiglu_grads(z1, z3, da)
            a_s[rest, cols] = act
            dz1_s[rest, cols] = dz1
            dz3_s[rest, cols] = dz3
        g1 = dot_tn(x_at[...], dz1_s[...])
        g3 = dot_tn(x_at[...], dz3_s[...])
        g2 = dot_tn(a_s[...], do_at[...])
        if first:
            o1_ref[0] = g1
            o3_ref[0] = g3
            o2_ref[0] = g2
        else:
            o1_ref[0] += g1
            o3_ref[0] += g3
            o2_ref[0] += g2

    xg_s[buf, j, :OWN, :] = own_x[0]
    do_s[buf, j, :OWN, :] = own_do[0]
    a_s[:OWN, :] = own_a[0]
    dz1_s[:OWN, :] = own_dz1[0]
    dz3_s[:OWN, :] = own_dz3[0]
    compute(xg_s.at[buf, j], do_s.at[buf, j], True)

    n_hot = jnp.int32(0)
    for b in range(SHARDS):
        list_s[b] = jnp.int32(0)
    for b in range(SHARDS):
        hit = hot_s[b] == e

        @pl.when(hit)
        def _(b=b, n_hot=n_hot):
            list_s[n_hot] = jnp.int32(b)
        n_hot = n_hot + hit.astype(jnp.int32)

    def hot_chunk(c, _):
        def hot_gather(k, _):
            pos = c * 4 + k
            b = list_s[pos]
            live = pos < n_hot
            mask = select(b, e, HOT, jnp.where(live, float(SLOT), 4096.0))
            sel = as_bf16(mask)
            rows = pl.ds(pl.multiple_of(k * HOT, HOT), HOT)
            xh_s[rows, :] = dot_nn(sel, x_s[b]).astype(BF16)
            gg = dot_nn(sel, g_s[b])
            p_col = jnp.sum(jnp.where(mask, gate_s[b, pl.ds(e, 1), :], 0.0), axis=1, keepdims=True)
            dh_s[rows, :] = (p_col * gg).astype(BF16)

            @pl.when(k < 2)
            def _():
                gg_s[rows, :] = gg.astype(BF16)
            return 0
        lax.fori_loop(0, 4, hot_gather, 0)
        compute(xh_s, dh_s, False)

        @pl.when((c == 0) & (list_s[0] < 2))
        def _():
            rows = slice(0, 2 * HOT)
            q, dx = own_grads(a_s[rows, :], dz1_s[rows, :], dz3_s[rows, :], gg_s[...], w1_ref[0], w3_ref[0], w2_ref[0])
            for k in range(2):
                b = list_s[k]

                @pl.when((k < n_hot) & (b < 2))
                def _(k=k, b=b):
                    part = slice(k * HOT, (k + 1) * HOT)
                    mask = select(b, e, HOT, float(SLOT))
                    s_ref[b] += dot_tn(as_bf16(mask), dx[part])
                    q_ref[b, pl.ds(i, 1), :] += jnp.sum(jnp.where(mask, q[part], 0.0), axis=0, keepdims=True)
        return 0

    lax.fori_loop(0, lax.div(n_hot + 3, 4), hot_chunk, 0)


def expert_pass(info, x_all, g_all, idx_all, w_router_t, s_part, q_part, own, w_gate, w_up, w_down):
    vmem = pl.BlockSpec(memory_space=pltpu.VMEM)
    hbm = pl.BlockSpec(memory_space=pl.ANY)
    up_spec = pl.BlockSpec((1, D, FF), lambda i, info: (i, 0, 0))
    down_spec = pl.BlockSpec((1, FF, D), lambda i, info: (i, 0, 0))
    own_d = pl.BlockSpec((1, OWN, D), lambda i, info: (i, 0, 0))
    own_f = pl.BlockSpec((1, OWN, FF), lambda i, info: (i, 0, 0))
    return pl.pallas_call(
        main_kernel,
        out_shape=(
            jax.ShapeDtypeStruct((E_LOC, D, FF), F32),
            jax.ShapeDtypeStruct((E_LOC, D, FF), F32),
            jax.ShapeDtypeStruct((E_LOC, FF, D), F32),
            jax.ShapeDtypeStruct((2, TOK, D), F32),
            jax.ShapeDtypeStruct((2, E_LOC, TOK), F32),
        ),
        grid_spec=pltpu.PrefetchScalarGridSpec(
            num_scalar_prefetch=1,
            grid=(E_LOC,),
            in_specs=[hbm, hbm, vmem, vmem, hbm, vmem, own_d, own_d, own_f, own_f, own_f, up_spec, up_spec, down_spec],
            out_specs=(up_spec, up_spec, down_spec, vmem, vmem),
            scratch_shapes=[
                pltpu.VMEM((SHARDS, TOK, D), BF16),
                pltpu.VMEM((SHARDS, TOK, D), BF16),
                pltpu.VMEM((SHARDS, EXPERTS, TOK), F32),
                pltpu.VMEM((SHARDS, EXPERTS, TOK), F32),
                pltpu.SMEM((SHARDS,), jnp.int32),
                pltpu.SMEM((SHARDS,), jnp.int32),
                pltpu.VMEM((2, GROUP, ROWS, D), BF16),
                pltpu.VMEM((2, GROUP, ROWS, D), BF16),
                pltpu.VMEM((ROWS, D), BF16),
                pltpu.VMEM((ROWS, D), BF16),
                pltpu.VMEM((2 * HOT, D), BF16),
                pltpu.VMEM((ROWS, FF), BF16),
                pltpu.VMEM((ROWS, FF), BF16),
                pltpu.VMEM((ROWS, FF), BF16),
                pltpu.SemaphoreType.DMA((3, SHARDS)),
            ],
        ),
        compiler_params=pltpu.CompilerParams(
            dimension_semantics=("arbitrary",), vmem_limit_bytes=VMEM_ALL),
        cost_estimate=pl.CostEstimate(flops=70_000_000_000, bytes_accessed=180_000_000, transcendentals=8_000_000),
        name="experts",
    )(info, x_all, g_all, idx_all, w_router_t, s_part, q_part, *own, w_gate, w_up, w_down)


def peer(step):
    chip = lax.axis_index("dp")
    core = lax.axis_index("ep")
    x_bit, y_bit = lax.rem(chip, 2), lax.div(chip, 2)
    if step & 2:
        x_bit = 1 - x_bit
    if step & 4:
        y_bit = 1 - y_bit
    if step & 1:
        core = 1 - core
    return {"dp": 2 * y_bit + x_bit, "ep": core}


def greet_all():
    barrier = pltpu.get_barrier_semaphore()
    for step in range(1, SHARDS):
        pl.semaphore_signal(barrier, inc=1, device_id=peer(step), device_id_type=MESH)
    pl.semaphore_wait(barrier, SHARDS - 1)


def share_kernel(x_ref, g_ref, idx_ref, wr_ref, w1_ref, w3_ref, w2_ref,
                 x_all, g_all, idx_all, s_ref, q_ref, gate_ref, own_x, own_do, own_a, own_dz1, own_dz3,
                 x_par, g_par, idx_par, code_s, gate_s, xg_s, do_s, gg_s, r_s, send, recv, local):
    i = pl.program_id(0)
    e = lax.axis_index("ep") * E_LOC + i
    j = lax.rem(i, GROUP)

    def copy(ref, into, sem, step):
        return pltpu.make_async_remote_copy(
            src_ref=ref, dst_ref=into, send_sem=send.at[sem], recv_sem=recv.at[sem],
            device_id=peer(step), device_id_type=MESH)

    own = [pltpu.make_async_copy(ref, into.at[0], local.at[n])
           for n, (ref, into) in enumerate(((x_ref, x_all), (g_ref, g_all), (idx_ref, idx_all)))]
    par = [pltpu.make_async_copy(ref, into.at[1], local.at[3 + n])
           for n, (ref, into) in enumerate(((x_par, x_all), (g_par, g_all), (idx_par, idx_all)))]
    x1, g1, id1 = copy(x_ref, x_par, 0, 1), copy(g_ref, g_par, 7, 1), copy(idx_ref, idx_par, 14, 1)
    ids = [copy(idx_ref, idx_all.at[k], 14 + k - 1, k) for k in range(2, SHARDS)]
    x2, g2 = copy(x_ref, x_all.at[2], 1, 2), copy(g_ref, g_all.at[2], 8, 2)
    g4, x4 = copy(g_ref, g_all.at[4], 10, 4), copy(x_ref, x_all.at[4], 3, 4)
    x6, g6 = copy(x_all.at[2], x_all.at[6], 5, 4), copy(g_all.at[4], g_all.at[6], 12, 2)
    x3, g3 = copy(x_all.at[2], x_all.at[3], 2, 1), copy(g_all.at[2], g_all.at[3], 9, 1)
    x5, g5 = copy(x_all.at[4], x_all.at[5], 4, 1), copy(g_all.at[4], g_all.at[5], 11, 1)
    x7, g7 = copy(x_all.at[6], x_all.at[7], 6, 1), copy(g_all.at[6], g_all.at[7], 13, 1)

    @pl.when(i == 0)
    def _():
        greet_all()
        for c in (id1, x2, g4, x1, g1, g2, x4, *ids):
            c.start()
        for c in own:
            c.start()
        s_ref[...] = jnp.zeros_like(s_ref)
        code, gates, _ = route_tables(x_ref[...], idx_ref[...], wr_ref[...])
        code_s[0] = code
        gate_s[0] = gates
        gate_ref[...] = gates
        id1.wait_recv()
        x1.wait_recv()
        g1.wait_recv()
        for c in par:
            c.start()
        code, gates, _ = route_tables(x_par[...], idx_par[...], wr_ref[...])
        code_s[1] = code
        gate_s[1] = gates

    @pl.when(i == FORWARD[0])
    def _():
        x2.wait_recv()
        g4.wait_recv()
        for c in (x6, g6, x3, g5):
            c.start()

    @pl.when(i == FORWARD[1])
    def _():
        g2.wait_recv()
        x4.wait_recv()
        g3.start()
        x5.start()

    @pl.when(i == FORWARD[2])
    def _():
        x6.wait_recv()
        x7.start()
        g6.wait_recv()
        g7.start()

    @pl.when(j == 0)
    def _():
        for b, (xb, gb) in enumerate(((x_ref, g_ref), (x_par, g_par))):
            masks = [slot_mask(code_s[b, pl.ds(e + jj, 1), :], SLOT, 0.0) for jj in range(GROUP)]
            sel = jnp.concatenate([as_bf16(m) for m in masks], axis=0)
            xg = dot_nn(sel, xb[...]).astype(BF16)
            gg = dot_nn(sel, gb[...])
            rows = slice(b * SLOT, (b + 1) * SLOT)
            for jj in range(GROUP):
                part = slice(jj * SLOT, (jj + 1) * SLOT)
                xg_s[jj, rows, :] = xg[part]
                gg_s[jj, rows, :] = gg[part].astype(BF16)
                p_col = jnp.sum(jnp.where(masks[jj], gate_s[b, pl.ds(e + jj, 1), :], 0.0), axis=1, keepdims=True)
                do_s[jj, rows, :] = (p_col * gg[part]).astype(BF16)

    z1 = dot_nn(xg_s[j], w1_ref[0])
    z3 = dot_nn(xg_s[j], w3_ref[0])
    da = dot_nt(do_s[j], w2_ref[0])
    act, dz1, dz3 = swiglu_grads(z1, z3, da)
    own_x[0] = xg_s[j]
    own_do[0] = do_s[j]
    own_a[0] = act
    own_dz1[0] = dz1
    own_dz3[0] = dz3
    o = dot_nn(act, w2_ref[0])
    q = jnp.sum(o * gg_s[j].astype(F32), axis=1, keepdims=True)
    for b in range(2):
        mask = slot_mask(code_s[b, pl.ds(e, 1), :], SLOT, 0.0)
        q_ref[b, pl.ds(i, 1), :] = jnp.sum(jnp.where(mask, q[b * SLOT:(b + 1) * SLOT], 0.0), axis=0, keepdims=True)
    odd = lax.rem(i, 2)
    dx_t = dot_nt(w1_ref[0], dz1) + dot_nt(w3_ref[0], dz3)
    r_s[:, pl.ds(pl.multiple_of(odd * OWN, OWN), OWN)] = dx_t.astype(BF16)

    @pl.when(odd == 1)
    def _():
        zero = jnp.zeros((SLOT, TOK), BF16)
        rows = []
        for ex in (e - 1, e):
            first, second = (as_bf16(slot_mask(code_s[b, pl.ds(ex, 1), :], SLOT, 0.0)) for b in range(2))
            rows += [jnp.concatenate([first, zero], axis=1), jnp.concatenate([zero, second], axis=1)]
        part = lax.dot_general(jnp.concatenate(rows, axis=0), r_s[...], (((0,), (1,)), ((), ())), preferred_element_type=F32)
        for b in range(2):
            s_ref[b] += part[b * TOK:(b + 1) * TOK]

    @pl.when(i == E_LOC - 1)
    def _():
        for c in (x3, g3, x5, g5, x7, g7, *ids):
            c.wait_recv()
        for c in (x1, g1, id1, x2, g2, g4, x4, x6, g6, x3, g3, x5, g5, x7, g7, *ids):
            c.wait_send()
        for c in own + par:
            c.wait()


def share_tokens(x_loc, dy_loc, idx_t, w_router_t, w_gate, w_up, w_down):
    vmem = pl.BlockSpec(memory_space=pltpu.VMEM)
    hbm = pl.BlockSpec(memory_space=pl.ANY)
    up_spec = pl.BlockSpec((1, D, FF), lambda i: (i, 0, 0))
    down_spec = pl.BlockSpec((1, FF, D), lambda i: (i, 0, 0))
    own_d = pl.BlockSpec((1, OWN, D), lambda i: (i, 0, 0))
    own_f = pl.BlockSpec((1, OWN, FF), lambda i: (i, 0, 0))
    return pl.pallas_call(
        share_kernel,
        out_shape=(
            jax.ShapeDtypeStruct((SHARDS, TOK, D), BF16),
            jax.ShapeDtypeStruct((SHARDS, TOK, D), BF16),
            jax.ShapeDtypeStruct((SHARDS, TOP, TOK), jnp.int32),
            jax.ShapeDtypeStruct((2, TOK, D), F32),
            jax.ShapeDtypeStruct((2, E_LOC, TOK), F32),
            jax.ShapeDtypeStruct((EXPERTS, TOK), F32),
            jax.ShapeDtypeStruct((E_LOC, OWN, D), BF16),
            jax.ShapeDtypeStruct((E_LOC, OWN, D), BF16),
            jax.ShapeDtypeStruct((E_LOC, OWN, FF), BF16),
            jax.ShapeDtypeStruct((E_LOC, OWN, FF), BF16),
            jax.ShapeDtypeStruct((E_LOC, OWN, FF), BF16),
        ),
        grid=(E_LOC,),
        in_specs=[vmem] * 4 + [up_spec, up_spec, down_spec],
        out_specs=(hbm, hbm, hbm, vmem, vmem, vmem, own_d, own_d, own_f, own_f, own_f),
        scratch_shapes=[
            pltpu.VMEM((TOK, D), BF16),
            pltpu.VMEM((TOK, D), BF16),
            pltpu.VMEM((TOP, TOK), jnp.int32),
            pltpu.VMEM((2, EXPERTS, TOK), F32),
            pltpu.VMEM((2, EXPERTS, TOK), F32),
            pltpu.VMEM((GROUP, OWN, D), BF16),
            pltpu.VMEM((GROUP, OWN, D), BF16),
            pltpu.VMEM((GROUP, OWN, D), BF16),
            pltpu.VMEM((D, 2 * OWN), BF16),
            pltpu.SemaphoreType.DMA((21,)),
            pltpu.SemaphoreType.DMA((21,)),
            pltpu.SemaphoreType.DMA((6,)),
        ],
        compiler_params=pltpu.CompilerParams(
            dimension_semantics=("arbitrary",), collective_id=0, has_side_effects=True, vmem_limit_bytes=VMEM_ALL),
        cost_estimate=pl.CostEstimate(flops=20_000_000_000, bytes_accessed=70_000_000, transcendentals=2_000_000),
        name="share",
    )(x_loc, dy_loc, idx_t, w_router_t, w_gate, w_up, w_down)


def tail_kernel(s_hbm, q_hbm, gate_hbm, x_hbm, wr_ref, gx_ref, gr_ref,
                s_own, s_got, q_own, q_got, gate_s, x_all, dl_all, send, recv, local):
    core = lax.axis_index("ep")

    def copy(ref, into, sem, step):
        return pltpu.make_async_remote_copy(
            src_ref=ref, dst_ref=into, send_sem=send.at[sem], recv_sem=recv.at[sem],
            device_id=peer(step), device_id_type=MESH)

    loads = [pltpu.make_async_copy(ref, into, local.at[n]) for n, (ref, into) in enumerate(
        ((q_hbm.at[0], q_own), (gate_hbm, gate_s), (s_hbm.at[0], s_own), (x_hbm, x_all)))]
    for c in loads:
        c.start()
    greet_all()
    q_copy = copy(q_hbm.at[1], q_got, 0, 1)
    s_copy = copy(s_hbm.at[1], s_got, 1, 1)
    q_copy.start()
    s_copy.start()
    loads[0].wait()
    loads[1].wait()
    q_copy.wait_recv()
    low = jnp.concatenate([q_own[...], q_got[...]], axis=0)
    high = jnp.concatenate([q_got[...], q_own[...]], axis=0)
    q = jnp.where(core == 0, low, high)
    p = gate_s[...]
    d_log = (p * (q - jnp.sum(p * q, axis=0, keepdims=True))).astype(BF16)
    dl_all[0] = d_log
    copies = [copy(dl_all.at[0], dl_all.at[k], 1 + k, k) for k in range(1, SHARDS)]
    for c in copies:
        c.start()
    du = dot_tn(d_log, wr_ref[...])
    loads[2].wait()
    s_copy.wait_recv()
    gx_ref[...] = (s_own[...] + s_got[...] + du).astype(BF16)
    loads[3].wait()
    total = dot_nn(d_log, x_all[0])
    for k in range(1, SHARDS):
        copies[k - 1].wait_recv()
        total += dot_nn(dl_all[k], x_all[k])
    gr_ref[...] = total
    q_copy.wait_send()
    s_copy.wait_send()
    for c in copies:
        c.wait_send()


def tail(dx_part, q_part, gates, x_all, w_router_t):
    vmem = pl.BlockSpec(memory_space=pltpu.VMEM)
    hbm = pl.BlockSpec(memory_space=pl.ANY)
    return pl.pallas_call(
        tail_kernel,
        out_shape=(jax.ShapeDtypeStruct((TOK, D), BF16), jax.ShapeDtypeStruct((EXPERTS, D), F32)),
        in_specs=[hbm] * 4 + [vmem],
        out_specs=(vmem, vmem),
        scratch_shapes=[
            pltpu.VMEM((TOK, D), F32),
            pltpu.VMEM((TOK, D), F32),
            pltpu.VMEM((E_LOC, TOK), F32),
            pltpu.VMEM((E_LOC, TOK), F32),
            pltpu.VMEM((EXPERTS, TOK), F32),
            pltpu.VMEM((SHARDS, TOK, D), BF16),
            pltpu.VMEM((SHARDS, EXPERTS, TOK), BF16),
            pltpu.SemaphoreType.DMA((9,)),
            pltpu.SemaphoreType.DMA((9,)),
            pltpu.SemaphoreType.DMA((4,)),
        ],
        compiler_params=pltpu.CompilerParams(collective_id=1, has_side_effects=True, vmem_limit_bytes=62_000_000),
        name="tail",
    )(dx_part, q_part, gates, x_all, w_router_t)


def solution(mesh):
    tok_spec = P(("dp", "ep"), None)
    exp_spec = P("ep", None, None)

    def device_step(x_loc, route_idx, w_router, w_gate, w_up, w_down, dy_loc):
        info = lax.axis_index("ep").astype(jnp.int32).reshape(1)
        w_router_t = w_router.T
        x_all, g_all, idx_all, dx_own, q_own, gates, *own = share_tokens(
            x_loc, dy_loc, route_idx.T, w_router_t, w_gate, w_up, w_down)
        g1, g3, g2, dx_part, q_part = expert_pass(
            info, x_all, g_all, idx_all, w_router_t, dx_own, q_own, own, w_gate, w_up, w_down)
        grad_x, grad_router_t = tail(dx_part, q_part, gates, x_all, w_router_t)
        return grad_x, g1, g3, g2, grad_router_t.T

    return jax.shard_map(device_step, mesh=mesh, in_specs=(tok_spec, tok_spec, P(), exp_spec, exp_spec, exp_spec, tok_spec), out_specs=(tok_spec, exp_spec, exp_spec, exp_spec, P()), check_vma=False)
```

```python
import jax
import jax.numpy as jnp
from jax import lax
from jax.experimental import pallas as pl
from jax.experimental.pallas import tpu as pltpu
from jax.sharding import PartitionSpec as P

D = 1024
FF = 512
EXPERTS = 32
TOP = 8
TOK = 256
SHARDS = 8
E_LOC = 16
SLOT = 64
GROUP = 4
ROWS = SHARDS * SLOT
HOT = 128
OWN = 2 * SLOT
FORWARD = (5, 9, 14)
VMEM_ALL = 67_000_000
CAP = 192
F32 = jnp.float32
BF16 = jnp.bfloat16
MESH = pl.DeviceIdType.MESH


def dot_nn(a, b):
    return lax.dot_general(a, b, (((1,), (0,)), ((), ())), preferred_element_type=F32)


def dot_nt(a, b):
    return lax.dot_general(a, b, (((1,), (1,)), ((), ())), preferred_element_type=F32)


def dot_tn(a, b):
    return lax.dot_general(a, b, (((0,), (0,)), ((), ())), preferred_element_type=F32)


def route_tables(x_s, idx_t, w_router_t):
    logits = dot_nt(w_router_t, x_s)
    e_iota = lax.broadcasted_iota(jnp.int32, (EXPERTS, TOK), 0)
    mask = e_iota == idx_t[0:1, :]
    for k in range(1, TOP):
        mask = mask | (e_iota == idx_t[k:k + 1, :])
    top = jnp.max(jnp.where(mask, logits, -jnp.inf), axis=0, keepdims=True)
    ex = jnp.where(mask, jnp.exp(jnp.where(mask, logits - top, 0.0)), 0.0)
    gates = ex / jnp.sum(ex, axis=0, keepdims=True)
    mask_f = jnp.where(mask, 1.0, 0.0)
    before = lax.broadcasted_iota(jnp.int32, (TOK, TOK), 0) < lax.broadcasted_iota(jnp.int32, (TOK, TOK), 1)
    rank = dot_nn(mask_f.astype(BF16), jnp.where(before, 1.0, 0.0).astype(BF16))
    code = jnp.where(mask, rank, -1.0)
    count = jnp.sum(mask_f, axis=1, keepdims=True)
    return code, gates, count


def slot_mask(code_row, rows, base):
    r_iota = lax.broadcasted_iota(jnp.int32, (rows, TOK), 0).astype(F32)
    return code_row - base == r_iota


def as_bf16(mask):
    return jnp.where(mask, 1.0, 0.0).astype(BF16)


def swiglu_grads(z1, z3, da):
    sig = jax.nn.sigmoid(z1)
    silu = z1 * sig
    act = (silu * z3).astype(BF16)
    dz1 = (da * z3 * sig * (1.0 + z1 * (1.0 - sig))).astype(BF16)
    dz3 = (da * silu).astype(BF16)
    return act, dz1, dz3


def own_grads(act, dz1, dz3, gg, w1, w3, w2):
    o = dot_nn(act, w2)
    q = jnp.sum(o * gg.astype(F32), axis=1, keepdims=True)
    dx = (dot_nt(dz1, w1) + dot_nt(dz3, w3)).astype(BF16)
    return q, dx


def main_kernel(info, x_hbm, g_hbm, idx_ref, wr_ref, s_hbm, q_in, own_x, own_do, own_a, own_dz1, own_dz3,
                w1_ref, w3_ref, w2_ref, o1_ref, o3_ref, o2_ref, s_ref, q_ref, gate_s,
                x_s, g_s, code_s, hot_s, list_s, xg_s, do_s, xh_s, dh_s, gg_s, a_s, dz1_s, dz3_s, sem):
    i = pl.program_id(0)
    e = info[0] * E_LOC + i
    j = lax.rem(i, GROUP)
    buf = lax.rem(lax.div(i, GROUP), 2)

    def load(ref, into, b, n):
        return pltpu.make_async_copy(ref.at[b], into.at[b], sem.at[n, b])

    s_load = pltpu.make_async_copy(s_hbm, s_ref, sem.at[2, 0])

    def select(b, ex, rows, base):
        return slot_mask(code_s[b, pl.ds(ex, 1), :], rows, base)

    def gather(b, first, into):
        masks = [select(b, first + jj, SLOT, 0.0) for jj in range(GROUP)]
        sel = jnp.concatenate([as_bf16(m) for m in masks], axis=0)
        xg = dot_nn(sel, x_s[b]).astype(BF16)
        gg = dot_nn(sel, g_s[b])
        row0 = pl.multiple_of(b * SLOT, SLOT)
        for jj in range(GROUP):
            part = slice(jj * SLOT, (jj + 1) * SLOT)
            xg_s[into, jj, pl.ds(row0, SLOT), :] = xg[part]
            p_col = jnp.sum(jnp.where(masks[jj], gate_s[b, pl.ds(first + jj, 1), :], 0.0), axis=1, keepdims=True)
            do_s[into, jj, pl.ds(row0, SLOT), :] = (p_col * gg[part]).astype(BF16)

    @pl.when(i == 0)
    def _():
        for b in range(SHARDS):
            load(x_hbm, x_s, b, 0).start()
            load(g_hbm, g_s, b, 1).start()
        s_load.start()

        def prep(b, _):
            load(x_hbm, x_s, b, 0).wait()
            code, gates, count = route_tables(x_s[b], idx_ref[b], wr_ref[...])
            code_s[b] = code
            gate_s[b] = gates
            e_col = lax.broadcasted_iota(jnp.int32, (EXPERTS, 1), 0).astype(F32)
            hot_s[b] = jnp.max(jnp.where(count > SLOT, e_col, -1.0)).astype(jnp.int32)
            load(g_hbm, g_s, b, 1).wait()
            return 0
        lax.fori_loop(0, SHARDS, prep, 0)
        q_ref[...] = q_in[...]

        def first_gather(b, _):
            gather(b, e, 0)
            return 0
        lax.fori_loop(2, SHARDS, first_gather, 0)
        s_load.wait()

    @pl.when((i < E_LOC - GROUP) & (j < 3))
    def _():
        for k in range(2):
            gather(2 + 2 * j + k, e - j + GROUP, 1 - buf)

    def compute(x_at, do_at, first):
        skip = OWN if first else 0
        rest = slice(skip, ROWS)
        for n in range(2):
            cols = slice(n * 256, (n + 1) * 256)
            z1 = dot_nn(x_at[rest, :], w1_ref[0, :, cols])
            z3 = dot_nn(x_at[rest, :], w3_ref[0, :, cols])
            da = dot_nt(do_at[rest, :], w2_ref[0, cols, :])
            act, dz1, dz3 = swiglu_grads(z1, z3, da)
            a_s[rest, cols] = act
            dz1_s[rest, cols] = dz1
            dz3_s[rest, cols] = dz3
        g1 = dot_tn(x_at[...], dz1_s[...])
        g3 = dot_tn(x_at[...], dz3_s[...])
        g2 = dot_tn(a_s[...], do_at[...])
        if first:
            o1_ref[0] = g1
            o3_ref[0] = g3
            o2_ref[0] = g2
        else:
            o1_ref[0] += g1
            o3_ref[0] += g3
            o2_ref[0] += g2

    xg_s[buf, j, :OWN, :] = own_x[0]
    do_s[buf, j, :OWN, :] = own_do[0]
    a_s[:OWN, :] = own_a[0]
    dz1_s[:OWN, :] = own_dz1[0]
    dz3_s[:OWN, :] = own_dz3[0]
    compute(xg_s.at[buf, j], do_s.at[buf, j], True)

    n_hot = jnp.int32(0)
    for b in range(SHARDS):
        list_s[b] = jnp.int32(0)
    for b in range(SHARDS):
        hit = hot_s[b] == e

        @pl.when(hit)
        def _(b=b, n_hot=n_hot):
            list_s[n_hot] = jnp.int32(b)
        n_hot = n_hot + hit.astype(jnp.int32)

    def hot_chunk(c, _):
        def hot_gather(k):
            pos = c * 4 + k
            b = list_s[pos]
            live = pos < n_hot
            mask = select(b, e, HOT, jnp.where(live, float(SLOT), 4096.0))
            sel = as_bf16(mask)
            rows = slice(k * HOT, (k + 1) * HOT)
            xh_s[rows, :] = dot_nn(sel, x_s[b]).astype(BF16)
            gg = dot_nn(sel, g_s[b])
            p_col = jnp.sum(jnp.where(mask, gate_s[b, pl.ds(e, 1), :], 0.0), axis=1, keepdims=True)
            dh_s[rows, :] = (p_col * gg).astype(BF16)

            if k < 2:
                gg_s[rows, :] = gg.astype(BF16)
        for k in range(4):
            hot_gather(k)
        compute(xh_s, dh_s, False)

        @pl.when((c == 0) & (list_s[0] < 2))
        def _():
            rows = slice(0, 2 * HOT)
            q, dx = own_grads(a_s[rows, :], dz1_s[rows, :], dz3_s[rows, :], gg_s[...], w1_ref[0], w3_ref[0], w2_ref[0])
            for k in range(2):
                b = list_s[k]

                @pl.when((k < n_hot) & (b < 2))
                def _(k=k, b=b):
                    part = slice(k * HOT, (k + 1) * HOT)
                    mask = select(b, e, HOT, float(SLOT))
                    s_ref[b] += dot_tn(as_bf16(mask), dx[part])
                    q_ref[b, pl.ds(i, 1), :] += jnp.sum(jnp.where(mask, q[part], 0.0), axis=0, keepdims=True)
        return 0

    lax.fori_loop(0, lax.div(n_hot + 3, 4), hot_chunk, 0)


def expert_pass(info, x_all, g_all, idx_all, w_router_t, s_part, q_part, own, w_gate, w_up, w_down):
    vmem = pl.BlockSpec(memory_space=pltpu.VMEM)
    hbm = pl.BlockSpec(memory_space=pl.ANY)
    up_spec = pl.BlockSpec((1, D, FF), lambda i, info: (i, 0, 0))
    down_spec = pl.BlockSpec((1, FF, D), lambda i, info: (i, 0, 0))
    own_d = pl.BlockSpec((1, OWN, D), lambda i, info: (i, 0, 0))
    own_f = pl.BlockSpec((1, OWN, FF), lambda i, info: (i, 0, 0))
    return pl.pallas_call(
        main_kernel,
        out_shape=(
            jax.ShapeDtypeStruct((E_LOC, D, FF), F32),
            jax.ShapeDtypeStruct((E_LOC, D, FF), F32),
            jax.ShapeDtypeStruct((E_LOC, FF, D), F32),
            jax.ShapeDtypeStruct((2, TOK, D), F32),
            jax.ShapeDtypeStruct((2, E_LOC, TOK), F32),
            jax.ShapeDtypeStruct((SHARDS, EXPERTS, TOK), F32),
        ),
        grid_spec=pltpu.PrefetchScalarGridSpec(
            num_scalar_prefetch=1,
            grid=(E_LOC,),
            in_specs=[hbm, hbm, vmem, vmem, hbm, vmem, own_d, own_d, own_f, own_f, own_f, up_spec, up_spec, down_spec],
            out_specs=(up_spec, up_spec, down_spec, vmem, vmem, vmem),
            scratch_shapes=[
                pltpu.VMEM((SHARDS, TOK, D), BF16),
                pltpu.VMEM((SHARDS, TOK, D), BF16),
                pltpu.VMEM((SHARDS, EXPERTS, TOK), F32),
                pltpu.SMEM((SHARDS,), jnp.int32),
                pltpu.SMEM((SHARDS,), jnp.int32),
                pltpu.VMEM((2, GROUP, ROWS, D), BF16),
                pltpu.VMEM((2, GROUP, ROWS, D), BF16),
                pltpu.VMEM((ROWS, D), BF16),
                pltpu.VMEM((ROWS, D), BF16),
                pltpu.VMEM((2 * HOT, D), BF16),
                pltpu.VMEM((ROWS, FF), BF16),
                pltpu.VMEM((ROWS, FF), BF16),
                pltpu.VMEM((ROWS, FF), BF16),
                pltpu.SemaphoreType.DMA((3, SHARDS)),
            ],
        ),
        compiler_params=pltpu.CompilerParams(
            dimension_semantics=("arbitrary",), vmem_limit_bytes=VMEM_ALL),
        cost_estimate=pl.CostEstimate(flops=70_000_000_000, bytes_accessed=180_000_000, transcendentals=8_000_000),
        name="experts",
    )(info, x_all, g_all, idx_all, w_router_t, s_part, q_part, *own, w_gate, w_up, w_down)


def peer(step):
    chip = lax.axis_index("dp")
    core = lax.axis_index("ep")
    x_bit, y_bit = lax.rem(chip, 2), lax.div(chip, 2)
    if step & 2:
        x_bit = 1 - x_bit
    if step & 4:
        y_bit = 1 - y_bit
    if step & 1:
        core = 1 - core
    return {"dp": 2 * y_bit + x_bit, "ep": core}


def greet_all():
    barrier = pltpu.get_barrier_semaphore()
    for step in range(1, SHARDS):
        pl.semaphore_signal(barrier, inc=1, device_id=peer(step), device_id_type=MESH)
    pl.semaphore_wait(barrier, SHARDS - 1)


def share_kernel(x_hbm, g_hbm, idx_ref, wr_ref, w1_hbm, w3_hbm, w2_hbm,
                 x_all, g_all, idx_all, s_ref, q_ref, own_x, own_do, own_a, own_dz1, own_dz3,
                 x_ref, g_ref, x_par, g_par, idx_par, code_s, gate_s, xg_s, do_s, gg_s, r_s, w1_s, w3_s, w2_s,
                 send, recv, local, w_sem):
    i = pl.program_id(0)
    e = lax.axis_index("ep") * E_LOC + i
    j = lax.rem(i, GROUP)

    def copy(ref, into, sem, step):
        return pltpu.make_async_remote_copy(
            src_ref=ref, dst_ref=into, send_sem=send.at[sem], recv_sem=recv.at[sem],
            device_id=peer(step), device_id_type=MESH)

    own = [pltpu.make_async_copy(ref, into.at[0], local.at[n])
           for n, (ref, into) in enumerate(((x_ref, x_all), (g_ref, g_all), (idx_ref, idx_all)))]
    par = [pltpu.make_async_copy(ref, into.at[1], local.at[3 + n])
           for n, (ref, into) in enumerate(((x_par, x_all), (g_par, g_all), (idx_par, idx_all)))]
    takes = [pltpu.make_async_copy(x_hbm, x_ref, local.at[6]), pltpu.make_async_copy(g_hbm, g_ref, local.at[7])]

    def weights(step, to):
        return [pltpu.make_async_copy(ref.at[step], into.at[to], w_sem.at[n, to])
                for n, (ref, into) in enumerate(((w1_hbm, w1_s), (w3_hbm, w3_s), (w2_hbm, w2_s)))]

    now = lax.rem(i, 2)
    x1, g1, id1 = copy(x_hbm, x_par, 0, 1), copy(g_hbm, g_par, 7, 1), copy(idx_ref, idx_par, 14, 1)
    ids = [copy(idx_ref, idx_all.at[k], 14 + k - 1, k) for k in range(2, SHARDS)]
    x2, g2 = copy(x_hbm, x_all.at[2], 1, 2), copy(g_hbm, g_all.at[2], 8, 2)
    g4, x4 = copy(g_hbm, g_all.at[4], 10, 4), copy(x_hbm, x_all.at[4], 3, 4)
    x6, g6 = copy(x_all.at[2], x_all.at[6], 5, 4), copy(g_all.at[4], g_all.at[6], 12, 2)
    x3, g3 = copy(x_all.at[2], x_all.at[3], 2, 1), copy(g_all.at[2], g_all.at[3], 9, 1)
    x5, g5 = copy(x_all.at[4], x_all.at[5], 4, 1), copy(g_all.at[4], g_all.at[5], 11, 1)
    x7, g7 = copy(x_all.at[6], x_all.at[7], 6, 1), copy(g_all.at[6], g_all.at[7], 13, 1)

    @pl.when(i == 0)
    def _():
        for c in takes:
            c.start()
        greet_all()
        for c in (x2, g4, id1, x1, g1, g2, x4, *ids):
            c.start()
        for c in weights(0, 0):
            c.start()
        for c in takes:
            c.wait()
        for c in own:
            c.start()
        s_ref[...] = jnp.zeros_like(s_ref)
        code, gates, _ = route_tables(x_ref[...], idx_ref[...], wr_ref[...])
        code_s[0] = code
        gate_s[0] = gates
        id1.wait_recv()
        x1.wait_recv()
        g1.wait_recv()
        for c in par:
            c.start()
        code, gates, _ = route_tables(x_par[...], idx_par[...], wr_ref[...])
        code_s[1] = code
        gate_s[1] = gates

    @pl.when(i == FORWARD[0])
    def _():
        x2.wait_recv()
        g4.wait_recv()
        for c in (x6, g6, x3, g5):
            c.start()

    @pl.when(i == FORWARD[1])
    def _():
        g2.wait_recv()
        x4.wait_recv()
        g3.start()
        x5.start()

    @pl.when(i == FORWARD[2])
    def _():
        x6.wait_recv()
        x7.start()
        g6.wait_recv()
        g7.start()

    @pl.when(j == 0)
    def _():
        for b, (xb, gb) in enumerate(((x_ref, g_ref), (x_par, g_par))):
            masks = [slot_mask(code_s[b, pl.ds(e + jj, 1), :], SLOT, 0.0) for jj in range(GROUP)]
            sel = jnp.concatenate([as_bf16(m) for m in masks], axis=0)
            xg = dot_nn(sel, xb[...]).astype(BF16)
            gg = dot_nn(sel, gb[...])
            rows = slice(b * SLOT, (b + 1) * SLOT)
            for jj in range(GROUP):
                part = slice(jj * SLOT, (jj + 1) * SLOT)
                xg_s[jj, rows, :] = xg[part]
                gg_s[jj, rows, :] = gg[part].astype(BF16)
                p_col = jnp.sum(jnp.where(masks[jj], gate_s[b, pl.ds(e + jj, 1), :], 0.0), axis=1, keepdims=True)
                do_s[jj, rows, :] = (p_col * gg[part]).astype(BF16)

    for c in weights(i, now):
        c.wait()

    @pl.when(i < E_LOC - 1)
    def _():
        for c in weights(i + 1, 1 - now):
            c.start()

    z1 = dot_nn(xg_s[j], w1_s[now])
    z3 = dot_nn(xg_s[j], w3_s[now])
    da = dot_nt(do_s[j], w2_s[now])
    act, dz1, dz3 = swiglu_grads(z1, z3, da)
    own_x[0] = xg_s[j]
    own_do[0] = do_s[j]
    own_a[0] = act
    own_dz1[0] = dz1
    own_dz3[0] = dz3
    o = dot_nn(act, w2_s[now])
    q = jnp.sum(o * gg_s[j].astype(F32), axis=1, keepdims=True)
    for b in range(2):
        mask = slot_mask(code_s[b, pl.ds(e, 1), :], SLOT, 0.0)
        q_ref[b, pl.ds(i, 1), :] = jnp.sum(jnp.where(mask, q[b * SLOT:(b + 1) * SLOT], 0.0), axis=0, keepdims=True)
    odd = lax.rem(i, 2)
    dx_t = dot_nt(w1_s[now], dz1) + dot_nt(w3_s[now], dz3)
    r_s[:, pl.ds(pl.multiple_of(odd * OWN, OWN), OWN)] = dx_t.astype(BF16)

    @pl.when(odd == 1)
    def _():
        zero = jnp.zeros((SLOT, TOK), BF16)
        rows = []
        for ex in (e - 1, e):
            first, second = (as_bf16(slot_mask(code_s[b, pl.ds(ex, 1), :], SLOT, 0.0)) for b in range(2))
            rows += [jnp.concatenate([first, zero], axis=1), jnp.concatenate([zero, second], axis=1)]
        part = lax.dot_general(jnp.concatenate(rows, axis=0), r_s[...], (((0,), (1,)), ((), ())), preferred_element_type=F32)
        for b in range(2):
            s_ref[b] += part[b * TOK:(b + 1) * TOK]

    @pl.when(i == E_LOC - 1)
    def _():
        for c in (x3, g3, x5, g5, x7, g7, *ids):
            c.wait_recv()
        for c in (x1, g1, id1, x2, g2, g4, x4, x6, g6, x3, g3, x5, g5, x7, g7, *ids):
            c.wait_send()
        for c in own + par:
            c.wait()


def share_tokens(x_loc, dy_loc, idx_t, w_router_t, w_gate, w_up, w_down):
    vmem = pl.BlockSpec(memory_space=pltpu.VMEM)
    hbm = pl.BlockSpec(memory_space=pl.ANY)
    own_d = pl.BlockSpec((1, OWN, D), lambda i: (i, 0, 0))
    own_f = pl.BlockSpec((1, OWN, FF), lambda i: (i, 0, 0))
    return pl.pallas_call(
        share_kernel,
        out_shape=(
            jax.ShapeDtypeStruct((SHARDS, TOK, D), BF16),
            jax.ShapeDtypeStruct((SHARDS, TOK, D), BF16),
            jax.ShapeDtypeStruct((SHARDS, TOP, TOK), jnp.int32),
            jax.ShapeDtypeStruct((2, TOK, D), F32),
            jax.ShapeDtypeStruct((2, E_LOC, TOK), F32),
            jax.ShapeDtypeStruct((E_LOC, OWN, D), BF16),
            jax.ShapeDtypeStruct((E_LOC, OWN, D), BF16),
            jax.ShapeDtypeStruct((E_LOC, OWN, FF), BF16),
            jax.ShapeDtypeStruct((E_LOC, OWN, FF), BF16),
            jax.ShapeDtypeStruct((E_LOC, OWN, FF), BF16),
        ),
        grid=(E_LOC,),
        in_specs=[hbm, hbm, vmem, vmem, hbm, hbm, hbm],
        out_specs=(hbm, hbm, hbm, vmem, vmem, own_d, own_d, own_f, own_f, own_f),
        scratch_shapes=[
            pltpu.VMEM((TOK, D), BF16),
            pltpu.VMEM((TOK, D), BF16),
            pltpu.VMEM((TOK, D), BF16),
            pltpu.VMEM((TOK, D), BF16),
            pltpu.VMEM((TOP, TOK), jnp.int32),
            pltpu.VMEM((2, EXPERTS, TOK), F32),
            pltpu.VMEM((2, EXPERTS, TOK), F32),
            pltpu.VMEM((GROUP, OWN, D), BF16),
            pltpu.VMEM((GROUP, OWN, D), BF16),
            pltpu.VMEM((GROUP, OWN, D), BF16),
            pltpu.VMEM((D, 2 * OWN), BF16),
            pltpu.VMEM((2, D, FF), BF16),
            pltpu.VMEM((2, D, FF), BF16),
            pltpu.VMEM((2, FF, D), BF16),
            pltpu.SemaphoreType.DMA((21,)),
            pltpu.SemaphoreType.DMA((21,)),
            pltpu.SemaphoreType.DMA((8,)),
            pltpu.SemaphoreType.DMA((3, 2)),
        ],
        compiler_params=pltpu.CompilerParams(
            dimension_semantics=("arbitrary",), collective_id=0, has_side_effects=True, vmem_limit_bytes=VMEM_ALL),
        cost_estimate=pl.CostEstimate(flops=20_000_000_000, bytes_accessed=70_000_000, transcendentals=2_000_000),
        name="share",
    )(x_loc, dy_loc, idx_t, w_router_t, w_gate, w_up, w_down)


def tail_kernel(s_hbm, q_hbm, gate_hbm, x_hbm, wr_ref, gx_ref, gr_ref,
                s_own, s_got, q_all, gate_s, x_all, send, recv, local):
    core = lax.axis_index("ep")

    def copy(ref, into, sem, step):
        return pltpu.make_async_remote_copy(
            src_ref=ref, dst_ref=into, send_sem=send.at[sem], recv_sem=recv.at[sem],
            device_id=peer(step), device_id_type=MESH)

    loads = [pltpu.make_async_copy(ref, into, local.at[n]) for n, (ref, into) in enumerate(
        ((q_hbm, q_all.at[0]), (gate_hbm, gate_s), (s_hbm.at[0], s_own), (x_hbm, x_all)))]
    for c in loads[:2]:
        c.start()
    greet_all()
    loads[0].wait()
    copies = [copy(q_all.at[0], q_all.at[k], k, k) for k in range(1, SHARDS)]
    for k in (6, 7, 2, 3, 4, 5, 1):
        copies[k - 1].start()
    s_copy = copy(s_hbm.at[1], s_got, 0, 1)
    s_copy.start()
    for c in loads[2:]:
        c.start()
    def d_logits(k, n):
        near, far = q_all[k, n], q_all[k + 1, 1 - n]
        low = jnp.concatenate([near, far], axis=0)
        high = jnp.concatenate([far, near], axis=0)
        q = jnp.where(core == 0, low, high)
        p = gate_s[k + n]
        return (p * (q - jnp.sum(p * q, axis=0, keepdims=True))).astype(BF16)

    loads[1].wait()
    copies[0].wait_recv()
    d_log = d_logits(0, 0)
    du = dot_tn(d_log, wr_ref[...])
    loads[2].wait()
    s_copy.wait_recv()
    gx_ref[...] = (s_own[...] + s_got[...] + du).astype(BF16)
    loads[3].wait()
    for k in range(2, SHARDS):
        copies[k - 1].wait_recv()
    every = jnp.concatenate([d_log] + [d_logits(k - k % 2, k % 2) for k in range(1, SHARDS)], axis=1)
    gr_ref[...] = dot_nn(every, x_all[...])
    s_copy.wait_send()
    for c in copies:
        c.wait_send()


def tail(dx_part, q_part, gates, x_all, w_router_t):
    vmem = pl.BlockSpec(memory_space=pltpu.VMEM)
    hbm = pl.BlockSpec(memory_space=pl.ANY)
    return pl.pallas_call(
        tail_kernel,
        out_shape=(jax.ShapeDtypeStruct((TOK, D), BF16), jax.ShapeDtypeStruct((EXPERTS, D), F32)),
        in_specs=[hbm] * 4 + [vmem],
        out_specs=(vmem, vmem),
        scratch_shapes=[
            pltpu.VMEM((TOK, D), F32),
            pltpu.VMEM((TOK, D), F32),
            pltpu.VMEM((SHARDS, 2, E_LOC, TOK), F32),
            pltpu.VMEM((SHARDS, EXPERTS, TOK), F32),
            pltpu.VMEM((SHARDS * TOK, D), BF16),
            pltpu.SemaphoreType.DMA((SHARDS,)),
            pltpu.SemaphoreType.DMA((SHARDS,)),
            pltpu.SemaphoreType.DMA((4,)),
        ],
        compiler_params=pltpu.CompilerParams(collective_id=1, has_side_effects=True, vmem_limit_bytes=62_000_000),
        name="tail",
    )(dx_part, q_part, gates, x_all.reshape(SHARDS * TOK, D), w_router_t)


def solution(mesh):
    tok_spec = P(("dp", "ep"), None)
    exp_spec = P("ep", None, None)

    def device_step(x_loc, route_idx, w_router, w_gate, w_up, w_down, dy_loc):
        info = lax.axis_index("ep").astype(jnp.int32).reshape(1)
        w_router_t = w_router.T
        x_all, g_all, idx_all, dx_own, q_own, *own = share_tokens(
            x_loc, dy_loc, route_idx.T, w_router_t, w_gate, w_up, w_down)
        g1, g3, g2, dx_part, q_part, gates = expert_pass(
            info, x_all, g_all, idx_all, w_router_t, dx_own, q_own, own, w_gate, w_up, w_down)
        grad_x, grad_router_t = tail(dx_part, q_part, gates, x_all, w_router_t)
        return grad_x, g1, g3, g2, grad_router_t.T

    return jax.shard_map(device_step, mesh=mesh, in_specs=(tok_spec, tok_spec, P(), exp_spec, exp_spec, exp_spec, tok_spec), out_specs=(tok_spec, exp_spec, exp_spec, exp_spec, P()), check_vma=False)
```

```python
import jax
import jax.numpy as jnp
from jax import lax
from jax.experimental import pallas as pl
from jax.experimental.pallas import tpu as pltpu
from jax.sharding import PartitionSpec as P

D = 1024
FF = 512
EXPERTS = 32
TOP = 8
TOK = 256
SHARDS = 8
E_LOC = 16
SLOT = 64
GROUP = 4
ROWS = SHARDS * SLOT
HOT = 128
OWN = 2 * SLOT
FORWARD = (5, 9, 14)
VMEM_ALL = 67_000_000
SWAP_VMEM = 55_000_000
FINISH_VMEM = 32_000_000
CAP = 192
F32 = jnp.float32
BF16 = jnp.bfloat16
MESH = pl.DeviceIdType.MESH


def dot_nn(a, b):
    return lax.dot_general(a, b, (((1,), (0,)), ((), ())), preferred_element_type=F32)


def dot_nt(a, b):
    return lax.dot_general(a, b, (((1,), (1,)), ((), ())), preferred_element_type=F32)


def dot_tn(a, b):
    return lax.dot_general(a, b, (((0,), (0,)), ((), ())), preferred_element_type=F32)


def route_tables(x_s, idx_t, w_router_t):
    logits = dot_nt(w_router_t, x_s)
    e_iota = lax.broadcasted_iota(jnp.int32, (EXPERTS, TOK), 0)
    mask = e_iota == idx_t[0:1, :]
    for k in range(1, TOP):
        mask = mask | (e_iota == idx_t[k:k + 1, :])
    top = jnp.max(jnp.where(mask, logits, -jnp.inf), axis=0, keepdims=True)
    ex = jnp.where(mask, jnp.exp(jnp.where(mask, logits - top, 0.0)), 0.0)
    gates = ex / jnp.sum(ex, axis=0, keepdims=True)
    mask_f = jnp.where(mask, 1.0, 0.0)
    before = lax.broadcasted_iota(jnp.int32, (TOK, TOK), 0) < lax.broadcasted_iota(jnp.int32, (TOK, TOK), 1)
    rank = dot_nn(mask_f.astype(BF16), jnp.where(before, 1.0, 0.0).astype(BF16))
    code = jnp.where(mask, rank, -1.0)
    count = jnp.sum(mask_f, axis=1, keepdims=True)
    return code, gates, count


def slot_mask(code_row, rows, base):
    r_iota = lax.broadcasted_iota(jnp.int32, (rows, TOK), 0).astype(F32)
    return code_row - base == r_iota


def as_bf16(mask):
    return jnp.where(mask, 1.0, 0.0).astype(BF16)


def swiglu_grads(z1, z3, da):
    sig = jax.nn.sigmoid(z1)
    silu = z1 * sig
    act = (silu * z3).astype(BF16)
    dz1 = (da * z3 * sig * (1.0 + z1 * (1.0 - sig))).astype(BF16)
    dz3 = (da * silu).astype(BF16)
    return act, dz1, dz3


def own_grads(act, dz1, dz3, gg, w1, w3, w2):
    o = dot_nn(act, w2)
    q = jnp.sum(o * gg.astype(F32), axis=1, keepdims=True)
    dx = (dot_nt(dz1, w1) + dot_nt(dz3, w3)).astype(BF16)
    return q, dx


def main_kernel(info, x_hbm, g_hbm, idx_ref, wr_ref, s_hbm, q_in, own_x, own_do, own_a, own_dz1, own_dz3,
                w1_ref, w3_ref, w2_ref, o1_ref, o3_ref, o2_ref, s_ref, q_ref, gate_s,
                x_s, g_s, code_s, hot_s, list_s, xg_s, do_s, xh_s, dh_s, gg_s, a_s, dz1_s, dz3_s, sem):
    i = pl.program_id(0)
    e = info[0] * E_LOC + i
    j = lax.rem(i, GROUP)
    buf = lax.rem(lax.div(i, GROUP), 2)

    def load(ref, into, b, n):
        return pltpu.make_async_copy(ref.at[b], into.at[b], sem.at[n, b])

    s_load = pltpu.make_async_copy(s_hbm, s_ref, sem.at[2, 0])

    def select(b, ex, rows, base):
        return slot_mask(code_s[b, pl.ds(ex, 1), :], rows, base)

    def gather(b, first, into):
        masks = [select(b, first + jj, SLOT, 0.0) for jj in range(GROUP)]
        sel = jnp.concatenate([as_bf16(m) for m in masks], axis=0)
        xg = dot_nn(sel, x_s[b]).astype(BF16)
        gg = dot_nn(sel, g_s[b])
        row0 = pl.multiple_of(b * SLOT, SLOT)
        for jj in range(GROUP):
            part = slice(jj * SLOT, (jj + 1) * SLOT)
            xg_s[into, jj, pl.ds(row0, SLOT), :] = xg[part]
            p_col = jnp.sum(jnp.where(masks[jj], gate_s[b, pl.ds(first + jj, 1), :], 0.0), axis=1, keepdims=True)
            do_s[into, jj, pl.ds(row0, SLOT), :] = (p_col * gg[part]).astype(BF16)

    @pl.when(i == 0)
    def _():
        for b in range(SHARDS):
            load(x_hbm, x_s, b, 0).start()
            load(g_hbm, g_s, b, 1).start()
        s_load.start()

        def prep(b, _):
            load(x_hbm, x_s, b, 0).wait()
            code, gates, count = route_tables(x_s[b], idx_ref[b], wr_ref[...])
            code_s[b] = code
            gate_s[b] = gates
            e_col = lax.broadcasted_iota(jnp.int32, (EXPERTS, 1), 0).astype(F32)
            hot_s[b] = jnp.max(jnp.where(count > SLOT, e_col, -1.0)).astype(jnp.int32)
            load(g_hbm, g_s, b, 1).wait()
            return 0
        lax.fori_loop(0, SHARDS, prep, 0)
        q_ref[...] = q_in[...]

        def first_gather(b, _):
            gather(b, e, 0)
            return 0
        lax.fori_loop(2, SHARDS, first_gather, 0)
        s_load.wait()

    @pl.when((i < E_LOC - GROUP) & (j < 3))
    def _():
        for k in range(2):
            gather(2 + 2 * j + k, e - j + GROUP, 1 - buf)

    def compute(x_at, do_at, first):
        skip = OWN if first else 0
        rest = slice(skip, ROWS)
        for n in range(2):
            cols = slice(n * 256, (n + 1) * 256)
            z1 = dot_nn(x_at[rest, :], w1_ref[0, :, cols])
            z3 = dot_nn(x_at[rest, :], w3_ref[0, :, cols])
            da = dot_nt(do_at[rest, :], w2_ref[0, cols, :])
            act, dz1, dz3 = swiglu_grads(z1, z3, da)
            a_s[rest, cols] = act
            dz1_s[rest, cols] = dz1
            dz3_s[rest, cols] = dz3
        g1 = dot_tn(x_at[...], dz1_s[...])
        g3 = dot_tn(x_at[...], dz3_s[...])
        g2 = dot_tn(a_s[...], do_at[...])
        if first:
            o1_ref[0] = g1
            o3_ref[0] = g3
            o2_ref[0] = g2
        else:
            o1_ref[0] += g1
            o3_ref[0] += g3
            o2_ref[0] += g2

    xg_s[buf, j, :OWN, :] = own_x[0]
    do_s[buf, j, :OWN, :] = own_do[0]
    a_s[:OWN, :] = own_a[0]
    dz1_s[:OWN, :] = own_dz1[0]
    dz3_s[:OWN, :] = own_dz3[0]
    compute(xg_s.at[buf, j], do_s.at[buf, j], True)

    n_hot = jnp.int32(0)
    for b in range(SHARDS):
        list_s[b] = jnp.int32(0)
    for b in range(SHARDS):
        hit = hot_s[b] == e

        @pl.when(hit)
        def _(b=b, n_hot=n_hot):
            list_s[n_hot] = jnp.int32(b)
        n_hot = n_hot + hit.astype(jnp.int32)

    def hot_chunk(c, _):
        def hot_gather(k):
            pos = c * 4 + k
            b = list_s[pos]
            live = pos < n_hot
            mask = select(b, e, HOT, jnp.where(live, float(SLOT), 4096.0))
            sel = as_bf16(mask)
            rows = slice(k * HOT, (k + 1) * HOT)
            xh_s[rows, :] = dot_nn(sel, x_s[b]).astype(BF16)
            gg = dot_nn(sel, g_s[b])
            p_col = jnp.sum(jnp.where(mask, gate_s[b, pl.ds(e, 1), :], 0.0), axis=1, keepdims=True)
            dh_s[rows, :] = (p_col * gg).astype(BF16)

            if k < 2:
                gg_s[rows, :] = gg.astype(BF16)
        for k in range(4):
            hot_gather(k)
        compute(xh_s, dh_s, False)

        @pl.when((c == 0) & (list_s[0] < 2))
        def _():
            rows = slice(0, 2 * HOT)
            q, dx = own_grads(a_s[rows, :], dz1_s[rows, :], dz3_s[rows, :], gg_s[...], w1_ref[0], w3_ref[0], w2_ref[0])
            for k in range(2):
                b = list_s[k]

                @pl.when((k < n_hot) & (b < 2))
                def _(k=k, b=b):
                    part = slice(k * HOT, (k + 1) * HOT)
                    mask = select(b, e, HOT, float(SLOT))
                    s_ref[b] += dot_tn(as_bf16(mask), dx[part])
                    q_ref[b, pl.ds(i, 1), :] += jnp.sum(jnp.where(mask, q[part], 0.0), axis=0, keepdims=True)
        return 0

    lax.fori_loop(0, lax.div(n_hot + 3, 4), hot_chunk, 0)


def expert_pass(info, x_all, g_all, idx_all, w_router_t, s_part, q_part, own, w_gate, w_up, w_down):
    vmem = pl.BlockSpec(memory_space=pltpu.VMEM)
    hbm = pl.BlockSpec(memory_space=pl.ANY)
    up_spec = pl.BlockSpec((1, D, FF), lambda i, info: (i, 0, 0))
    down_spec = pl.BlockSpec((1, FF, D), lambda i, info: (i, 0, 0))
    own_d = pl.BlockSpec((1, OWN, D), lambda i, info: (i, 0, 0))
    own_f = pl.BlockSpec((1, OWN, FF), lambda i, info: (i, 0, 0))
    return pl.pallas_call(
        main_kernel,
        out_shape=(
            jax.ShapeDtypeStruct((E_LOC, D, FF), F32),
            jax.ShapeDtypeStruct((E_LOC, D, FF), F32),
            jax.ShapeDtypeStruct((E_LOC, FF, D), F32),
            jax.ShapeDtypeStruct((2, TOK, D), F32),
            jax.ShapeDtypeStruct((2, E_LOC, TOK), F32),
            jax.ShapeDtypeStruct((SHARDS, EXPERTS, TOK), F32),
        ),
        grid_spec=pltpu.PrefetchScalarGridSpec(
            num_scalar_prefetch=1,
            grid=(E_LOC,),
            in_specs=[hbm, hbm, vmem, vmem, hbm, vmem, own_d, own_d, own_f, own_f, own_f, up_spec, up_spec, down_spec],
            out_specs=(up_spec, up_spec, down_spec, vmem, vmem, vmem),
            scratch_shapes=[
                pltpu.VMEM((SHARDS, TOK, D), BF16),
                pltpu.VMEM((SHARDS, TOK, D), BF16),
                pltpu.VMEM((SHARDS, EXPERTS, TOK), F32),
                pltpu.SMEM((SHARDS,), jnp.int32),
                pltpu.SMEM((SHARDS,), jnp.int32),
                pltpu.VMEM((2, GROUP, ROWS, D), BF16),
                pltpu.VMEM((2, GROUP, ROWS, D), BF16),
                pltpu.VMEM((ROWS, D), BF16),
                pltpu.VMEM((ROWS, D), BF16),
                pltpu.VMEM((2 * HOT, D), BF16),
                pltpu.VMEM((ROWS, FF), BF16),
                pltpu.VMEM((ROWS, FF), BF16),
                pltpu.VMEM((ROWS, FF), BF16),
                pltpu.SemaphoreType.DMA((3, SHARDS)),
            ],
        ),
        compiler_params=pltpu.CompilerParams(
            dimension_semantics=("arbitrary",), vmem_limit_bytes=VMEM_ALL),
        cost_estimate=pl.CostEstimate(flops=70_000_000_000, bytes_accessed=180_000_000, transcendentals=8_000_000),
        name="experts",
    )(info, x_all, g_all, idx_all, w_router_t, s_part, q_part, *own, w_gate, w_up, w_down)


def peer(step):
    chip = lax.axis_index("dp")
    core = lax.axis_index("ep")
    x_bit, y_bit = lax.rem(chip, 2), lax.div(chip, 2)
    if step & 2:
        x_bit = 1 - x_bit
    if step & 4:
        y_bit = 1 - y_bit
    if step & 1:
        core = 1 - core
    return {"dp": 2 * y_bit + x_bit, "ep": core}


def greet_all():
    barrier = pltpu.get_barrier_semaphore()
    for step in range(1, SHARDS):
        pl.semaphore_signal(barrier, inc=1, device_id=peer(step), device_id_type=MESH)
    pl.semaphore_wait(barrier, SHARDS - 1)


def share_kernel(x_hbm, g_hbm, idx_ref, wr_ref, w1_hbm, w3_hbm, w2_hbm,
                 x_all, g_all, idx_all, s_ref, q_ref, own_x, own_do, own_a, own_dz1, own_dz3,
                 x_ref, g_ref, x_par, g_par, idx_par, code_s, gate_s, xg_s, do_s, gg_s, r_s, w1_s, w3_s, w2_s,
                 send, recv, local, w_sem):
    i = pl.program_id(0)
    e = lax.axis_index("ep") * E_LOC + i
    j = lax.rem(i, GROUP)

    def copy(ref, into, sem, step):
        return pltpu.make_async_remote_copy(
            src_ref=ref, dst_ref=into, send_sem=send.at[sem], recv_sem=recv.at[sem],
            device_id=peer(step), device_id_type=MESH)

    own = [pltpu.make_async_copy(ref, into.at[0], local.at[n])
           for n, (ref, into) in enumerate(((x_ref, x_all), (g_ref, g_all), (idx_ref, idx_all)))]
    par = [pltpu.make_async_copy(ref, into.at[1], local.at[3 + n])
           for n, (ref, into) in enumerate(((x_par, x_all), (g_par, g_all), (idx_par, idx_all)))]
    takes = [pltpu.make_async_copy(x_hbm, x_ref, local.at[6]), pltpu.make_async_copy(g_hbm, g_ref, local.at[7])]

    def weights(step, to):
        return [pltpu.make_async_copy(ref.at[step], into.at[to], w_sem.at[n, to])
                for n, (ref, into) in enumerate(((w1_hbm, w1_s), (w3_hbm, w3_s), (w2_hbm, w2_s)))]

    now = lax.rem(i, 2)
    x1, g1, id1 = copy(x_hbm, x_par, 0, 1), copy(g_hbm, g_par, 7, 1), copy(idx_ref, idx_par, 14, 1)
    ids = [copy(idx_ref, idx_all.at[k], 14 + k - 1, k) for k in range(2, SHARDS)]
    x2, g2 = copy(x_hbm, x_all.at[2], 1, 2), copy(g_hbm, g_all.at[2], 8, 2)
    g4, x4 = copy(g_hbm, g_all.at[4], 10, 4), copy(x_hbm, x_all.at[4], 3, 4)
    x6, g6 = copy(x_all.at[2], x_all.at[6], 5, 4), copy(g_all.at[4], g_all.at[6], 12, 2)
    x3, g3 = copy(x_all.at[2], x_all.at[3], 2, 1), copy(g_all.at[2], g_all.at[3], 9, 1)
    x5, g5 = copy(x_all.at[4], x_all.at[5], 4, 1), copy(g_all.at[4], g_all.at[5], 11, 1)
    x7, g7 = copy(x_all.at[6], x_all.at[7], 6, 1), copy(g_all.at[6], g_all.at[7], 13, 1)

    @pl.when(i == 0)
    def _():
        for c in takes:
            c.start()
        greet_all()
        for c in (x2, g4, id1, x1, g1, g2, x4, *ids):
            c.start()
        for c in weights(0, 0):
            c.start()
        for c in takes:
            c.wait()
        for c in own:
            c.start()
        s_ref[...] = jnp.zeros_like(s_ref)
        code, gates, _ = route_tables(x_ref[...], idx_ref[...], wr_ref[...])
        code_s[0] = code
        gate_s[0] = gates
        id1.wait_recv()
        x1.wait_recv()
        g1.wait_recv()
        for c in par:
            c.start()
        code, gates, _ = route_tables(x_par[...], idx_par[...], wr_ref[...])
        code_s[1] = code
        gate_s[1] = gates

    @pl.when(i == FORWARD[0])
    def _():
        x2.wait_recv()
        g4.wait_recv()
        for c in (x6, g6, x3, g5):
            c.start()

    @pl.when(i == FORWARD[1])
    def _():
        g2.wait_recv()
        x4.wait_recv()
        g3.start()
        x5.start()

    @pl.when(i == FORWARD[2])
    def _():
        x6.wait_recv()
        x7.start()
        g6.wait_recv()
        g7.start()

    @pl.when(j == 0)
    def _():
        for b, (xb, gb) in enumerate(((x_ref, g_ref), (x_par, g_par))):
            masks = [slot_mask(code_s[b, pl.ds(e + jj, 1), :], SLOT, 0.0) for jj in range(GROUP)]
            sel = jnp.concatenate([as_bf16(m) for m in masks], axis=0)
            xg = dot_nn(sel, xb[...]).astype(BF16)
            gg = dot_nn(sel, gb[...])
            rows = slice(b * SLOT, (b + 1) * SLOT)
            for jj in range(GROUP):
                part = slice(jj * SLOT, (jj + 1) * SLOT)
                xg_s[jj, rows, :] = xg[part]
                gg_s[jj, rows, :] = gg[part].astype(BF16)
                p_col = jnp.sum(jnp.where(masks[jj], gate_s[b, pl.ds(e + jj, 1), :], 0.0), axis=1, keepdims=True)
                do_s[jj, rows, :] = (p_col * gg[part]).astype(BF16)

    for c in weights(i, now):
        c.wait()

    @pl.when(i < E_LOC - 1)
    def _():
        for c in weights(i + 1, 1 - now):
            c.start()

    z1 = dot_nn(xg_s[j], w1_s[now])
    z3 = dot_nn(xg_s[j], w3_s[now])
    da = dot_nt(do_s[j], w2_s[now])
    act, dz1, dz3 = swiglu_grads(z1, z3, da)
    own_x[0] = xg_s[j]
    own_do[0] = do_s[j]
    own_a[0] = act
    own_dz1[0] = dz1
    own_dz3[0] = dz3
    o = dot_nn(act, w2_s[now])
    q = jnp.sum(o * gg_s[j].astype(F32), axis=1, keepdims=True)
    for b in range(2):
        mask = slot_mask(code_s[b, pl.ds(e, 1), :], SLOT, 0.0)
        q_ref[b, pl.ds(i, 1), :] = jnp.sum(jnp.where(mask, q[b * SLOT:(b + 1) * SLOT], 0.0), axis=0, keepdims=True)
    odd = lax.rem(i, 2)
    dx_t = dot_nt(w1_s[now], dz1) + dot_nt(w3_s[now], dz3)
    r_s[:, pl.ds(pl.multiple_of(odd * OWN, OWN), OWN)] = dx_t.astype(BF16)

    @pl.when(odd == 1)
    def _():
        zero = jnp.zeros((SLOT, TOK), BF16)
        rows = []
        for ex in (e - 1, e):
            first, second = (as_bf16(slot_mask(code_s[b, pl.ds(ex, 1), :], SLOT, 0.0)) for b in range(2))
            rows += [jnp.concatenate([first, zero], axis=1), jnp.concatenate([zero, second], axis=1)]
        part = lax.dot_general(jnp.concatenate(rows, axis=0), r_s[...], (((0,), (1,)), ((), ())), preferred_element_type=F32)
        for b in range(2):
            s_ref[b] += part[b * TOK:(b + 1) * TOK]

    @pl.when(i == E_LOC - 1)
    def _():
        for c in (x3, g3, x5, g5, x7, g7, *ids):
            c.wait_recv()
        for c in (x1, g1, id1, x2, g2, g4, x4, x6, g6, x3, g3, x5, g5, x7, g7, *ids):
            c.wait_send()
        for c in own + par:
            c.wait()


def share_tokens(x_loc, dy_loc, idx_t, w_router_t, w_gate, w_up, w_down):
    vmem = pl.BlockSpec(memory_space=pltpu.VMEM)
    hbm = pl.BlockSpec(memory_space=pl.ANY)
    own_d = pl.BlockSpec((1, OWN, D), lambda i: (i, 0, 0))
    own_f = pl.BlockSpec((1, OWN, FF), lambda i: (i, 0, 0))
    return pl.pallas_call(
        share_kernel,
        out_shape=(
            jax.ShapeDtypeStruct((SHARDS, TOK, D), BF16),
            jax.ShapeDtypeStruct((SHARDS, TOK, D), BF16),
            jax.ShapeDtypeStruct((SHARDS, TOP, TOK), jnp.int32),
            jax.ShapeDtypeStruct((2, TOK, D), F32),
            jax.ShapeDtypeStruct((2, E_LOC, TOK), F32),
            jax.ShapeDtypeStruct((E_LOC, OWN, D), BF16),
            jax.ShapeDtypeStruct((E_LOC, OWN, D), BF16),
            jax.ShapeDtypeStruct((E_LOC, OWN, FF), BF16),
            jax.ShapeDtypeStruct((E_LOC, OWN, FF), BF16),
            jax.ShapeDtypeStruct((E_LOC, OWN, FF), BF16),
        ),
        grid=(E_LOC,),
        in_specs=[hbm, hbm, vmem, vmem, hbm, hbm, hbm],
        out_specs=(hbm, hbm, hbm, vmem, vmem, own_d, own_d, own_f, own_f, own_f),
        scratch_shapes=[
            pltpu.VMEM((TOK, D), BF16),
            pltpu.VMEM((TOK, D), BF16),
            pltpu.VMEM((TOK, D), BF16),
            pltpu.VMEM((TOK, D), BF16),
            pltpu.VMEM((TOP, TOK), jnp.int32),
            pltpu.VMEM((2, EXPERTS, TOK), F32),
            pltpu.VMEM((2, EXPERTS, TOK), F32),
            pltpu.VMEM((GROUP, OWN, D), BF16),
            pltpu.VMEM((GROUP, OWN, D), BF16),
            pltpu.VMEM((GROUP, OWN, D), BF16),
            pltpu.VMEM((D, 2 * OWN), BF16),
            pltpu.VMEM((2, D, FF), BF16),
            pltpu.VMEM((2, D, FF), BF16),
            pltpu.VMEM((2, FF, D), BF16),
            pltpu.SemaphoreType.DMA((21,)),
            pltpu.SemaphoreType.DMA((21,)),
            pltpu.SemaphoreType.DMA((8,)),
            pltpu.SemaphoreType.DMA((3, 2)),
        ],
        compiler_params=pltpu.CompilerParams(
            dimension_semantics=("arbitrary",), collective_id=0, has_side_effects=True, vmem_limit_bytes=VMEM_ALL),
        cost_estimate=pl.CostEstimate(flops=20_000_000_000, bytes_accessed=70_000_000, transcendentals=2_000_000),
        name="share",
    )(x_loc, dy_loc, idx_t, w_router_t, w_gate, w_up, w_down)


def swap_kernel(q_ref, s_hbm, q_all, s_got, send, recv, local):
    def copy(ref, into, sem, step):
        return pltpu.make_async_remote_copy(
            src_ref=ref, dst_ref=into, send_sem=send.at[sem], recv_sem=recv.at[sem],
            device_id=peer(step), device_id_type=MESH)

    greet_all()
    copies = [copy(q_ref, q_all.at[k], k, k) for k in range(1, SHARDS)]
    for k in (6, 7, 2, 3, 4, 5, 1):
        copies[k - 1].start()
    s_copy = copy(s_hbm.at[1], s_got, 0, 1)
    s_copy.start()
    own = pltpu.make_async_copy(q_ref, q_all.at[0], local)
    own.start()
    own.wait()
    for c in (*copies, s_copy):
        c.wait_recv()
    for c in (*copies, s_copy):
        c.wait_send()


def swap(dx_part, q_part):
    vmem = pl.BlockSpec(memory_space=pltpu.VMEM)
    hbm = pl.BlockSpec(memory_space=pl.ANY)
    return pl.pallas_call(
        swap_kernel,
        out_shape=(jax.ShapeDtypeStruct((SHARDS, 2, E_LOC, TOK), F32), jax.ShapeDtypeStruct((TOK, D), F32)),
        in_specs=[vmem, hbm],
        out_specs=(vmem, hbm),
        scratch_shapes=[
            pltpu.SemaphoreType.DMA((SHARDS,)),
            pltpu.SemaphoreType.DMA((SHARDS,)),
            pltpu.SemaphoreType.DMA,
        ],
        compiler_params=pltpu.CompilerParams(collective_id=1, has_side_effects=True, vmem_limit_bytes=SWAP_VMEM),
        cost_estimate=pl.CostEstimate(flops=5_000_000_000, bytes_accessed=3_000_000, transcendentals=0),
        name="swap",
    )(q_part, dx_part)


def finish_kernel(info, s_own, s_got, q_all, gates, x_ref, wr_ref, gx_ref, gr_ref):
    def d_logits(k, n):
        near, far = q_all[k, n], q_all[k + 1, 1 - n]
        low = jnp.concatenate([near, far], axis=0)
        high = jnp.concatenate([far, near], axis=0)
        q = jnp.where(info[0] == 0, low, high)
        p = gates[k + n]
        return (p * (q - jnp.sum(p * q, axis=0, keepdims=True))).astype(BF16)

    every = [d_logits(k - k % 2, k % 2) for k in range(SHARDS)]
    gx_ref[...] = (s_own[0] + s_got[...] + dot_tn(every[0], wr_ref[...])).astype(BF16)
    gr_ref[...] = dot_nn(jnp.concatenate(every, axis=1), x_ref[...])


def finish(info, dx_part, s_got, q_all, gates, x_all, w_router_t):
    def whole(*shape):
        return pl.BlockSpec(shape, lambda i, info: (0,) * len(shape))
    return pl.pallas_call(
        finish_kernel,
        out_shape=(jax.ShapeDtypeStruct((TOK, D), BF16), jax.ShapeDtypeStruct((EXPERTS, D), F32)),
        grid_spec=pltpu.PrefetchScalarGridSpec(
            num_scalar_prefetch=1,
            grid=(1,),
            in_specs=[whole(1, TOK, D), whole(TOK, D), whole(SHARDS, 2, E_LOC, TOK), whole(SHARDS, EXPERTS, TOK),
                      whole(SHARDS * TOK, D), whole(EXPERTS, D)],
            out_specs=(whole(TOK, D), whole(EXPERTS, D)),
        ),
        compiler_params=pltpu.CompilerParams(vmem_limit_bytes=FINISH_VMEM),
        cost_estimate=pl.CostEstimate(flops=1_000_000_000, bytes_accessed=7_000_000, transcendentals=0),
        name="finish",
    )(info, dx_part, s_got, q_all, gates, x_all.reshape(SHARDS * TOK, D), w_router_t)


def solution(mesh):
    tok_spec = P(("dp", "ep"), None)
    exp_spec = P("ep", None, None)

    def device_step(x_loc, route_idx, w_router, w_gate, w_up, w_down, dy_loc):
        info = lax.axis_index("ep").astype(jnp.int32).reshape(1)
        w_router_t = w_router.T
        x_all, g_all, idx_all, dx_own, q_own, *own = share_tokens(
            x_loc, dy_loc, route_idx.T, w_router_t, w_gate, w_up, w_down)
        g1, g3, g2, dx_part, q_part, gates = expert_pass(
            info, x_all, g_all, idx_all, w_router_t, dx_own, q_own, own, w_gate, w_up, w_down)
        q_all, s_got = swap(dx_part, q_part)
        grad_x, grad_router_t = finish(info, dx_part, s_got, q_all, gates, x_all, w_router_t)
        return grad_x, g1, g3, g2, grad_router_t.T

    return jax.shard_map(device_step, mesh=mesh, in_specs=(tok_spec, tok_spec, P(), exp_spec, exp_spec, exp_spec, tok_spec), out_specs=(tok_spec, exp_spec, exp_spec, exp_spec, P()), check_vma=False)
```
